32 devices in a mesh: vid: 4 (over z), th: 4 (over x, core), tw: 2 (over y).
Axes of the slice: x: 2, y: 2, z: 4, core: 2. Of those that a mesh axis runs over, the one named last changes fastest.
Arguments:
- queries: bfloat16 [16, 32, 6, 3072], P('vid', 'th', 'tw'), parts along dimension 0, may hold values from -70 to 70
- video_kv: bfloat16 [2, 16, 32, 6, 3072], P(None, 'vid', 'th', 'tw'), parts along dimension 1, may hold values from -6 to 6
- text_kv: bfloat16 [2, 904, 3072], P(None, 'vid', 'tw'), parts along dimension 1, may hold values from -6 to 6
- time_embed: bfloat16 [2048], P('vid'), parts along dimension 0, may hold values from -6 to 6
- gate_weight: bfloat16 [512, 3072], P(None, 'tw'), may hold values from -0.25 to 0.25
- window_extent: int32 [48, 2], replicated, may hold values from 1 to 3
- tile_valid: int32 [16, 2, 2], P('vid'), parts along dimension 0, may hold values from 2 to 8, as said below
Outputs:
- gated: bfloat16 [16, 32, 6, 3072], P('vid', 'th', 'tw'), parts along dimension 0
The draws below stay inside these ranges and needn't reach their ends.
There are 4 independent parts, one for each index of `vid`. The reference program is written for one: setup_inputs(seed, part) draws one part's arguments, and reference() takes and returns one part's arrays. A program takes and returns all parts, laid end to end along the dimension named above; an argument that names none is the same for every part. Nothing has to cross between parts.
Inputs may be any that keep to these rules, and one draw needn't show every extreme that they name: Tile (i, j) holds tokens in its leading tile_valid[i, j, 0] of 8 rows and leading tile_valid[i, j, 1] of 3 columns; its other slots are padding. Some tile is full in every draw.
All inputs are finite; a program needn't handle non-finite values.
Results may differ from the reference program's by a relative error of at most 0.0063.
Values may be sent and summed in bfloat16 or wider, within the bound.
No kernel may reach another device: no remote copies, remote signals or barrier semaphores. Data moves between devices by JAX's collectives and lax.ppermute only.
A program may use at most 128 MiB of HBM per device.

```python
import jax
import jax.numpy as jnp
from jax import lax

HEADS = 48
HEAD_DIM = 64
D = 3072
TXT = 226
TEMB = 512
FR = 4
TH_DEV = 8
TW_DEV = 3
HALO = 3
N_TH = 4
N_TW = 2


def clipped(rand_key, full_shape):
    return jnp.clip(jax.random.normal(rand_key, full_shape, jnp.float32), -6.0, 6.0)


def shared_fields(base_key):
    folded = jax.random.fold_in(base_key, 7301)
    key_q, key_k, key_v, key_tk, key_tv = jax.random.split(folded, 5)
    model_width = HEADS * HEAD_DIM
    full_shape = (FR, TH_DEV * N_TH, TW_DEV * N_TW, model_width)
    text_shape = (TXT, model_width)
    queries = clipped(key_q, full_shape)
    video_keys = clipped(key_k, full_shape)
    values = clipped(key_v, full_shape)
    text_keys = clipped(key_tk, text_shape)
    text_values = clipped(key_tv, text_shape)
    return (queries, jnp.stack([video_keys, values]), jnp.stack([text_keys, text_values]))


def draw_queries(key, part):
    return shared_fields(key)[0].astype(jnp.bfloat16)


def draw_video_kv(key, part):
    return shared_fields(key)[1].astype(jnp.bfloat16)


def draw_text_kv(key, part):
    return shared_fields(key)[2].astype(jnp.bfloat16)


def draw_tile_valid(key, part):
    folded = jax.random.fold_in(key, 5519)
    key_rows, key_cols, key_full = jax.random.split(folded, 3)
    valid_rows = jax.random.randint(key_rows, (N_TH, N_TW), 2, TH_DEV + 1)
    valid_cols = jax.random.randint(key_cols, (N_TH, N_TW), 2, TW_DEV + 1)
    full_tile = jax.random.randint(key_full, (), 0, N_TH * N_TW)
    chosen = jnp.arange(N_TH * N_TW).reshape(N_TH, N_TW) == full_tile
    valid_rows = jnp.where(chosen, TH_DEV, valid_rows)
    valid_cols = jnp.where(chosen, TW_DEV, valid_cols)
    return jnp.stack([valid_rows, valid_cols], axis=-1).astype(jnp.int32)


def set_ends(entries, own_key, smallest, largest):
    place = [jax.random.randint(jax.random.fold_in(own_key, axis), (), 0, length) for axis, length in enumerate(entries.shape)]
    main_axis = entries.shape.index(max(entries.shape))
    beside = place[:main_axis] + [(place[main_axis] + 1) % entries.shape[main_axis]] + place[main_axis + 1:]
    return entries.at[tuple(place)].set(smallest).at[tuple(beside)].set(largest)


def shard_levels(key, shape, shards, smallest, high):
    def one(axis_at, blocks):
        heights = jax.random.uniform(jax.random.fold_in(jax.random.fold_in(key, 6), axis_at), (blocks,), jnp.float32, smallest / len(shards), high / len(shards))
        return jnp.repeat(jnp.exp(heights), shape[axis_at] // blocks).reshape((-1,) + (1,) * (len(shape) - axis_at - 1))

    level = one(*shards[0])
    for cut in shards[1:]:
        level = level * one(*cut)
    return level


def normal_values(own_key, shape, spread, limit, cuts=(), held_as=jnp.bfloat16):
    level = shard_levels(own_key, shape, cuts, -0.22, 0.18) if cuts else 1.0
    values = jax.random.normal(own_key, shape, jnp.float32) * spread * level
    return jnp.minimum(jnp.maximum(values, -limit), limit).astype(held_as)


def setup_inputs(seed: int = 0, part: int = 0) -> dict:
    seeds = jax.random.split(jax.random.key(seed), 8)
    part_keys = jax.random.split(jax.random.fold_in(seeds[7], part), 8)
    queries = draw_queries(jax.random.fold_in(jax.random.fold_in(seeds[7], part), 71), part)
    video_kv = draw_video_kv(jax.random.fold_in(jax.random.fold_in(seeds[7], part), 71), part)
    text_kv = draw_text_kv(jax.random.fold_in(jax.random.fold_in(seeds[7], part), 71), part)
    time_embed = normal_values(part_keys[3], (TEMB,), 1.0, 6.0)
    gate_weight = normal_values(seeds[4], (TEMB, D), TEMB ** -0.5, 0.25, ((1, 2),))
    window_extent = set_ends(jax.random.randint(seeds[5], (HEADS, 2), 1, HALO + 1), jax.random.fold_in(seeds[5], 1), 1, HALO).astype(jnp.int32)
    tile_valid = draw_tile_valid(jax.random.fold_in(jax.random.fold_in(seeds[7], part), 71), part)
    return dict(queries=queries, video_kv=video_kv, text_kv=text_kv, time_embed=time_embed, gate_weight=gate_weight, window_extent=window_extent, tile_valid=tile_valid)


NEG = -1e30


def text_part(query_rows, text_keys, text_values, score_scale):
    scores = jnp.einsum("nhd,thd->nht", query_rows.astype(jnp.float32), text_keys.astype(jnp.float32)) * score_scale
    maximum = jnp.max(scores, axis=-1)
    exp_terms = jnp.exp(scores - maximum[..., None])
    totals = jnp.sum(exp_terms, axis=-1)
    rounded = lax.optimization_barrier(exp_terms.astype(jnp.bfloat16)).astype(jnp.float32)
    partial_value = jnp.einsum("nht,thd->nhd", rounded, text_values.astype(jnp.float32))
    return partial_value, maximum, totals


def video_part(query_rows, video_keys, video_values, key_ok, window_extent, frames, tile_rows, tile_cols, score_scale):
    count_q, head_count, head_depth = query_rows.shape
    span_rows = tile_rows + 2 * HALO
    span_cols = tile_cols + 2 * HALO
    row_gap = jnp.abs(jnp.arange(span_rows, dtype=jnp.int32)[None, :] - jnp.arange(tile_rows, dtype=jnp.int32)[:, None] - HALO)
    col_gap = jnp.abs(jnp.arange(span_cols, dtype=jnp.int32)[None, :] - jnp.arange(tile_cols, dtype=jnp.int32)[:, None] - HALO)
    near_row = row_gap[None] <= window_extent[:, 0][:, None, None]
    near_col = col_gap[None] <= window_extent[:, 1][:, None, None]
    allowed = near_row[:, None, :, None, None, :, None] & near_col[:, None, None, :, None, None, :] & key_ok[None, None, None, None, None, :, :]
    scores = jnp.einsum("nhd,khd->hnk", query_rows.astype(jnp.float32), video_keys.astype(jnp.float32)) * score_scale
    scores = jnp.where(allowed, scores.reshape(head_count, frames, tile_rows, tile_cols, frames, span_rows, span_cols), NEG)
    maximum = jnp.max(scores, axis=(4, 5, 6))
    exp_terms = jnp.where(allowed, jnp.exp(scores - maximum[..., None, None, None]), 0.0)
    totals = jnp.sum(exp_terms, axis=(4, 5, 6))
    rounded = lax.optimization_barrier(exp_terms.reshape(head_count, count_q, -1).astype(jnp.bfloat16)).astype(jnp.float32)
    partial_value = jnp.einsum("hnk,khd->nhd", rounded, video_values.astype(jnp.float32))
    return partial_value, maximum.reshape(head_count, count_q), totals.reshape(head_count, count_q)


def combine(video_out, video_max, video_total, text_out, text_max, text_total):
    max_v = video_max.T
    total_v = video_total.T
    joint_max = jnp.maximum(max_v, text_max)
    scale_v = jnp.exp(max_v - joint_max)
    scale_t = jnp.exp(text_max - joint_max)
    denom = total_v * scale_v + text_total * scale_t
    return (video_out * scale_v[..., None] + text_out * scale_t[..., None]) / denom[..., None]


def reference(queries, video_kv, text_kv, time_embed, gate_weight, window_extent, tile_valid):
    frames, grid_rows, grid_cols, model_width = queries.shape
    tile_rows = grid_rows // N_TH
    tile_cols = grid_cols // N_TW
    head_count = model_width // HEAD_DIM
    score_scale = HEAD_DIM ** -0.5
    span_rows = tile_rows + 2 * HALO
    span_cols = tile_cols + 2 * HALO
    mod_in = jax.nn.silu(time_embed.astype(jnp.float32)).astype(jnp.bfloat16)
    gate_full = jnp.dot(mod_in[None, :], gate_weight, preferred_element_type=jnp.float32)[0].astype(jnp.bfloat16)
    row_ids = jnp.arange(grid_rows, dtype=jnp.int32)
    col_ids = jnp.arange(grid_cols, dtype=jnp.int32)
    tile_limit = tile_valid[(row_ids // tile_rows)[:, None], (col_ids // tile_cols)[None, :]]
    token_ok = ((row_ids % tile_rows)[:, None] < tile_limit[..., 0]) & ((col_ids % tile_cols)[None, :] < tile_limit[..., 1])
    token_ok = token_ok.astype(jnp.int32)
    padded_kv = jnp.pad(video_kv, ((0, 0), (0, 0), (HALO, HALO), (HALO, HALO), (0, 0)))
    padded_ok = jnp.pad(token_ok, HALO)
    text_keys = text_kv[0].reshape(-1, head_count, HEAD_DIM)
    text_values = text_kv[1].reshape(-1, head_count, HEAD_DIM)

    def one_tile(tile_index):
        tile_row = tile_index // N_TW
        tile_col = tile_index % N_TW
        row_start = (tile_row * tile_rows).astype(jnp.int32)
        col_start = (tile_col * tile_cols).astype(jnp.int32)
        anchor = jnp.zeros((), jnp.int32)
        query_block = lax.dynamic_slice(queries, (anchor, row_start, col_start, anchor), (frames, tile_rows, tile_cols, model_width))
        kv_block = lax.dynamic_slice(padded_kv, (anchor, anchor, row_start, col_start, anchor), (2, frames, span_rows, span_cols, model_width))
        key_ok = lax.dynamic_slice(padded_ok, (row_start, col_start), (span_rows, span_cols)) > 0
        query_ok = lax.dynamic_slice(token_ok, (row_start, col_start), (tile_rows, tile_cols)) > 0
        query_rows = query_block.reshape(-1, head_count, HEAD_DIM)
        video_keys = kv_block[0].reshape(-1, head_count, HEAD_DIM)
        video_values = kv_block[1].reshape(-1, head_count, HEAD_DIM)
        video_out, video_max, video_total = video_part(query_rows, video_keys, video_values, key_ok, window_extent, frames, tile_rows, tile_cols, score_scale)
        text_out, text_max, text_total = text_part(query_rows, text_keys, text_values, score_scale)
        attended = combine(video_out, video_max, video_total, text_out, text_max, text_total)
        attended = attended.reshape(frames, tile_rows, tile_cols, model_width)
        result = jnp.where(query_ok[None, :, :, None], gate_full.astype(jnp.float32) * attended, 0.0)
        return result.astype(jnp.bfloat16)

    tile_out = lax.map(one_tile, jnp.arange(N_TH * N_TW, dtype=jnp.int32))
    tile_out = tile_out.reshape(N_TH, N_TW, frames, tile_rows, tile_cols, model_width)
    tile_out = jnp.transpose(tile_out, (2, 0, 3, 1, 4, 5))
    return tile_out.reshape(frames, grid_rows, grid_cols, model_width)
```

```python
import math
from functools import partial

import jax
import jax.numpy as jnp
import numpy as np
from jax import lax
from jax.experimental import pallas as pl
from jax.experimental.pallas import tpu as pltpu
from jax.sharding import PartitionSpec as P

HEAD_DIM = 64
HALO = 3


NEG = -1e30


def extended(cells, sides, width):
    for axis, dim in sides:
        count = lax.axis_size(axis)
        ends = count - 1
        head = lax.slice_in_dim(cells, 0, width, axis=dim)
        tail = lax.slice_in_dim(cells, cells.shape[dim] - width, cells.shape[dim], axis=dim)
        cells = jnp.concatenate(
            [
                lax.ppermute(tail, axis, [(i, (i + 1) % count) for i in range(ends)]),
                cells,
                lax.ppermute(head, axis, [((i + 1) % count, i) for i in range(ends)]),
            ],
            axis=dim,
        )
    return cells


def key_validity(tile_valid, row_at, col_at, tile_rows, tile_cols):
    tiles_down = tile_valid.shape[0]
    tiles_across = tile_valid.shape[1]
    glob_row = row_at * tile_rows + jnp.arange(tile_rows + 2 * HALO, dtype=jnp.int32) - HALO
    glob_col = col_at * tile_cols + jnp.arange(tile_cols + 2 * HALO, dtype=jnp.int32) - HALO
    tile_row = jnp.floor_divide(glob_row, tile_rows)
    tile_col = jnp.floor_divide(glob_col, tile_cols)
    pick_row = (tile_row[:, None] == jnp.arange(tiles_down, dtype=jnp.int32)[None, :]).astype(
        jnp.float32
    )
    pick_col = (tile_col[:, None] == jnp.arange(tiles_across, dtype=jnp.int32)[None, :]).astype(
        jnp.float32
    )
    table = tile_valid.astype(jnp.float32)
    high = lax.Precision.HIGHEST
    limit_rows = jnp.dot(
        jnp.dot(pick_row, table[..., 0], precision=high), pick_col.T, precision=high
    )
    limit_cols = jnp.dot(
        jnp.dot(pick_row, table[..., 1], precision=high), pick_col.T, precision=high
    )
    local_row = (glob_row - tile_row * tile_rows).astype(jnp.float32)
    local_col = (glob_col - tile_col * tile_cols).astype(jnp.float32)
    return (local_row[:, None] < limit_rows) & (local_col[None, :] < limit_cols)


def video_part(
    query_rows,
    video_keys,
    video_values,
    key_ok,
    window_extent,
    frames,
    tile_rows,
    tile_cols,
    score_scale,
):
    count_q, head_count, head_depth = query_rows.shape
    count_k = video_keys.shape[0]
    span_rows = tile_rows + 2 * HALO
    span_cols = tile_cols + 2 * HALO
    per_turn = math.gcd(head_count, 4)
    query_ids = jnp.arange(count_q, dtype=jnp.int32)
    key_ids = jnp.arange(count_k, dtype=jnp.int32)
    query_row = query_ids // tile_cols % tile_rows
    query_col = query_ids % tile_cols
    key_row = key_ids // span_cols % span_rows
    key_col = key_ids % span_cols
    row_gap = jnp.abs(key_row[None, :] - query_row[:, None] - HALO)
    col_gap = jnp.abs(key_col[None, :] - query_col[:, None] - HALO)
    key_flat = jnp.tile(key_ok.reshape(-1), frames)

    def one_group(turn_index, carry):
        video_out, video_max, video_total = carry
        first_head = jnp.asarray(turn_index, jnp.int32) * per_turn
        query_part = lax.dynamic_slice_in_dim(query_rows, first_head, per_turn, 1)
        key_part = lax.dynamic_slice_in_dim(video_keys, first_head, per_turn, 1)
        value_part = lax.dynamic_slice_in_dim(video_values, first_head, per_turn, 1)
        extents = lax.dynamic_slice_in_dim(window_extent, first_head, per_turn, 0)
        allowed = (
            (row_gap[None] <= extents[:, 0][:, None, None])
            & (col_gap[None] <= extents[:, 1][:, None, None])
            & key_flat[None, None, :]
        )
        scores = (
            jnp.einsum("nhd,khd->hnk", query_part, key_part, preferred_element_type=jnp.float32)
            * score_scale
        )
        scores = jnp.where(allowed, scores, NEG)
        maximum = jnp.max(scores, axis=-1)
        exp_terms = jnp.where(allowed, jnp.exp(scores - maximum[..., None]), 0.0)
        totals = jnp.sum(exp_terms, axis=-1)
        weights = exp_terms.astype(jnp.bfloat16)
        partial_value = jnp.einsum(
            "hnk,khd->nhd", weights, value_part, preferred_element_type=jnp.float32
        )
        video_out = lax.dynamic_update_slice_in_dim(video_out, partial_value, first_head, 1)
        video_max = lax.dynamic_update_slice_in_dim(video_max, maximum, first_head, 0)
        video_total = lax.dynamic_update_slice_in_dim(video_total, totals, first_head, 0)
        return (video_out, video_max, video_total)

    initial = (
        jnp.zeros((count_q, head_count, head_depth), jnp.float32),
        jnp.zeros((head_count, count_q), jnp.float32),
        jnp.zeros((head_count, count_q), jnp.float32),
    )
    return lax.fori_loop(0, head_count // per_turn, one_group, initial)


def text_part(query_rows, text_keys, text_values, score_scale):
    scores = (
        jnp.einsum("nhd,thd->nht", query_rows, text_keys, preferred_element_type=jnp.float32)
        * score_scale
    )
    maximum = jnp.max(scores, axis=-1)
    exp_terms = jnp.exp(scores - maximum[..., None])
    totals = jnp.sum(exp_terms, axis=-1)
    partial_value = jnp.einsum(
        "nht,thd->nhd",
        exp_terms.astype(jnp.bfloat16),
        text_values,
        preferred_element_type=jnp.float32,
    )
    return (partial_value, maximum, totals)


def combine(video_out, video_max, video_total, text_out, text_max, text_total):
    max_v = video_max.T
    total_v = video_total.T
    joint_max = jnp.maximum(max_v, text_max)
    scale_v = jnp.exp(max_v - joint_max)
    scale_t = jnp.exp(text_max - joint_max)
    denom = total_v * scale_v + text_total * scale_t
    return (video_out * scale_v[..., None] + text_out * scale_t[..., None]) / denom[..., None]


def attend_tile(
    query_block,
    kv_block,
    text_keys,
    text_values,
    extents,
    gate_vec,
    key_ok,
    tile_rows,
    tile_cols,
    score_scale,
):
    frames = query_block.shape[0]
    width = query_block.shape[3]
    head_count = width // HEAD_DIM
    query_rows = query_block.reshape(-1, head_count, HEAD_DIM)
    video_keys = kv_block[0].reshape(-1, head_count, HEAD_DIM)
    video_values = kv_block[1].reshape(-1, head_count, HEAD_DIM)
    video_out, video_max, video_total = video_part(
        query_rows,
        video_keys,
        video_values,
        key_ok,
        extents,
        frames,
        tile_rows,
        tile_cols,
        score_scale,
    )
    text_out, text_max, text_total = text_part(query_rows, text_keys, text_values, score_scale)
    attended = combine(video_out, video_max, video_total, text_out, text_max, text_total)
    attended = attended.reshape(frames, tile_rows, tile_cols, width)
    query_ok = key_ok[HALO : HALO + tile_rows, HALO : HALO + tile_cols]
    result = jnp.where(query_ok[None, :, :, None], gate_vec.astype(jnp.float32) * attended, 0.0)
    return result.astype(jnp.bfloat16)


def general_body(queries, video_kv, text_kv, time_embed, gate_weight, window_extent, tile_valid):
    frames, tile_rows, tile_cols, model_width = queries.shape
    head_count = model_width // HEAD_DIM
    score_scale = HEAD_DIM ** (-0.5)
    text_count = text_kv.shape[1]
    row_at = lax.axis_index("th")
    col_at = lax.axis_index("tw")
    mod_in = jax.nn.silu(time_embed.astype(jnp.float32)).astype(jnp.bfloat16)
    gate_part = jnp.dot(mod_in[None, :], gate_weight, preferred_element_type=jnp.float32)[0].astype(
        jnp.bfloat16
    )
    padded = extended(video_kv, (("th", 2), ("tw", 3)), HALO)
    text_full, gate_full = (
        lax.all_gather(text_kv, "tw", axis=2, tiled=True),
        lax.all_gather(gate_part, "tw", axis=0, tiled=True),
    )
    text_keys = text_full[0].reshape(text_count, head_count, HEAD_DIM)
    text_values = text_full[1].reshape(text_count, head_count, HEAD_DIM)
    key_ok = key_validity(tile_valid, row_at, col_at, tile_rows, tile_cols)
    return attend_tile(
        queries,
        padded,
        text_keys,
        text_values,
        window_extent,
        gate_full,
        key_ok,
        tile_rows,
        tile_cols,
        score_scale,
    )


LANES = 128
CHUNKS = (8, 4)
UNROLL = 2
VMEM_LIMIT = 16 * 2**20


def pack_kernel(q_ref, kv_ref, *refs, moves):
    outs, sems = refs[:-1], refs[-1]
    col_at = lax.axis_index("tw")
    half = q_ref.shape[2] // 2
    copies = []
    for at, (source, first, out, slot, other) in enumerate(moves):
        to = outs[out].at[slot]
        side = 1 - col_at if other else col_at
        lanes = pl.ds(pl.multiple_of(side * half + first, LANES), to.shape[2])
        ref = q_ref if source == 0 else kv_ref
        copies.append(pltpu.make_async_copy(ref.at[:, :, lanes], to, sems.at[at]))
    for copy in copies:
        copy.start()
    for copy in copies:
        copy.wait()


def pack(q, kv, shapes, moves, name):
    return pl.pallas_call(
        partial(pack_kernel, moves=moves),
        out_shape=[jax.ShapeDtypeStruct(shape, q.dtype) for shape in shapes],
        in_specs=[pl.BlockSpec(memory_space=pltpu.HBM)] * 2,
        out_specs=[pl.BlockSpec(memory_space=pltpu.VMEM)] * len(shapes),
        scratch_shapes=[pltpu.SemaphoreType.DMA((len(moves),))],
        compiler_params=pltpu.CompilerParams(vmem_limit_bytes=VMEM_LIMIT),
        name=name,
    )(q, kv)


def cut_edges(select_ref, keys_values, bottom_ref, top_ref):
    edge = bottom_ref.shape[1]
    for part in (0, 1):
        rows = lax.dot_general(
            select_ref[...],
            keys_values[part],
            (((1,), (0,)), ((), ())),
            preferred_element_type=jnp.float32,
        ).astype(jnp.bfloat16)
        bottom_ref[part] = rows[:edge]
        top_ref[part] = rows[edge:]


def edges_kernel(select_ref, peer_ref, *refs):
    bottom_ref, top_ref = refs[-2:]
    cut_edges(select_ref, (peer_ref[1], peer_ref[2]), bottom_ref, top_ref)


def prepare_kernel(
    valid_ref,
    select_ref,
    key_ref,
    query_ref,
    time_ref,
    weight_ref,
    kv_ref,
    bottom_ref,
    top_ref,
    bias_ref,
    gate_ref,
    ok_ref,
    *,
    tile_cols,
    tiles_down,
):
    row_at = lax.axis_index("th")
    col_at = lax.axis_index("tw")
    cut_edges(select_ref, (kv_ref[0], kv_ref[1]), bottom_ref, top_ref)
    key_row, key_local, key_col, key_block = (key_ref[i : i + 1] for i in range(4))
    query_row, query_col, query_peer = (query_ref[:, i : i + 1] for i in range(3))
    key_peer = key_block % 2
    row_limit = jnp.zeros_like(key_row)
    col_limit = jnp.zeros_like(key_row)
    query_limits = []
    for at, step in enumerate((0, -1, 1)):
        tile_row = row_at + step
        inside = (tile_row >= 0) & (tile_row < tiles_down)
        tile_row = jnp.clip(tile_row, 0, tiles_down - 1)
        for peer in (0, 1):
            side = 1 - col_at if peer else col_at
            rows = jnp.where(inside, valid_ref[side, 0, tile_row], 0)
            cols = valid_ref[side, 1, tile_row]
            block = 2 * at + peer
            row_limit = jnp.where(key_block == block, rows, row_limit)
            col_limit = jnp.where(key_block == block, cols, col_limit)
            if step == 0:
                query_limits.append((rows, cols))
    key_ok = (key_local < row_limit) & (key_col < col_limit)
    key_at = key_col + tile_cols * jnp.where(key_peer > 0, 1 - col_at, col_at)
    query_at = query_col + tile_cols * jnp.where(query_peer > 0, 1 - col_at, col_at)
    row_gap = jnp.abs(query_row - key_row)
    col_gap = jnp.where(key_ok, jnp.abs(query_at - key_at), 2 * HALO + 1)
    for rows in range(HALO):
        for cols in range(HALO):
            near = (row_gap <= rows + 1) & (col_gap <= cols + 1)
            bias_ref[rows * HALO + cols] = jnp.where(near, 0.0, NEG)
    row_limit = jnp.where(query_peer > 0, query_limits[1][0], query_limits[0][0])
    col_limit = jnp.where(query_peer > 0, query_limits[1][1], query_limits[0][1])
    query_ok = (query_row < row_limit) & (query_col < col_limit)
    ok_ref[...] = jnp.broadcast_to(jnp.where(query_ok, 1.0, 0.0), ok_ref.shape)
    step = time_ref[...].astype(jnp.float32)
    step = (step / (1.0 + jnp.exp(-step))).astype(jnp.bfloat16)
    gate = jnp.dot(step, weight_ref[...], preferred_element_type=jnp.float32)
    gate = gate.astype(jnp.bfloat16).astype(jnp.float32)
    for pair in range(gate_ref.shape[0]):
        gate_ref[pair] = gate[0:1, pair * LANES : (pair + 1) * LANES]


def attend_kernel(
    extent_ref,
    mine_q_ref,
    mine_kv_ref,
    peer_ref,
    above_mine_ref,
    below_mine_ref,
    above_peer_ref,
    below_peer_ref,
    text_ref,
    bias_ref,
    gate_ref,
    ok_ref,
    own_out_ref,
    peer_out_ref,
    key_ref,
    value_ref,
    *,
    first_pair,
    pairs,
    unroll,
    text_count,
    score_scale,
):
    count = mine_q_ref.shape[1]
    edge = above_mine_ref.shape[1]
    near = 2 * count + 4 * edge
    first_head = lax.axis_index("tw") * (2 * gate_ref.shape[0])
    left = lax.broadcasted_iota(jnp.int32, (1, LANES), 1) < HEAD_DIM
    zero = jnp.zeros((), jnp.bfloat16)
    one = jnp.ones((), jnp.bfloat16)
    text_rows = text_ref.shape[1]
    text_bias = jnp.where(
        lax.broadcasted_iota(jnp.int32, (1, text_rows), 1) < text_count, 0.0, NEG
    )

    def one_pair(turn, slot):
        here = pl.ds(pl.multiple_of(turn * LANES, LANES), LANES)
        whole = pl.ds(pl.multiple_of((first_pair + turn) * LANES, LANES), LANES)
        for part, into in ((0, key_ref.at[slot]), (1, value_ref.at[slot])):
            into[0:count] = mine_kv_ref[part, :, whole]
            into[count : 2 * count] = peer_ref[1 + part, :, here]
            at = 2 * count
            for ref, lanes in (
                (above_mine_ref, whole),
                (above_peer_ref, here),
                (below_mine_ref, whole),
                (below_peer_ref, here),
            ):
                into[at : at + edge] = ref[part, :, lanes]
                at += edge
            into[near:] = text_ref[part, :, whole]
        queries = jnp.concatenate([mine_q_ref[0, :, whole], peer_ref[0, :, here]], 0)
        queries = queries * jnp.asarray(score_scale, jnp.bfloat16)
        queries = jnp.concatenate([jnp.where(left, queries, zero), jnp.where(left, zero, queries)], 0)
        both = lax.dot_general(
            queries, key_ref[slot], (((1,), (1,)), ((), ())), preferred_element_type=jnp.float32
        )
        values = value_ref[slot]
        outs = []
        for side in (0, 1):
            head = first_head + 2 * (first_pair + turn) + side
            reach_rows = jnp.clip(extent_ref[0, head], 1, HALO) - 1
            reach_cols = jnp.clip(extent_ref[1, head], 1, HALO) - 1
            bias = bias_ref[reach_rows * HALO + reach_cols]
            scores = both[2 * count * side : 2 * count * (side + 1)]
            scores = jnp.concatenate([scores[:, :near] + bias, scores[:, near:] + text_bias], 1)
            top = jnp.max(scores, axis=-1, keepdims=True)
            weights = jnp.exp(scores - top).astype(jnp.bfloat16)
            summed = jnp.where(left, values, one) if side == 0 else jnp.where(left, one, values)
            outs.append(
                lax.dot_general(
                    weights, summed, (((1,), (0,)), ((), ())), preferred_element_type=jnp.float32
                )
            )
        total = pltpu.roll(jnp.where(left, outs[1], outs[0]), HEAD_DIM, 1)
        attended = jnp.where(left, outs[0], outs[1]) / total
        gated = jnp.where(ok_ref[...] > 0.0, attended * gate_ref[first_pair + turn], 0.0)
        gated = gated.astype(jnp.bfloat16)
        own_out_ref[:, here] = gated[:count]
        peer_out_ref[:, here] = gated[count:]

    def some_pairs(turn, carry):
        for slot in range(unroll):
            one_pair(turn * unroll + slot, slot)
        return carry

    lax.fori_loop(0, pairs // unroll, some_pairs, 0)


def place_kernel(*refs, moves):
    ins, out_ref, sems = refs[:-2], refs[-2], refs[-1]
    col_at = lax.axis_index("tw")
    half = out_ref.shape[1] // 2
    copies = []
    for at, (source, first, other) in enumerate(moves):
        side = 1 - col_at if other else col_at
        ref = ins[source]
        lanes = pl.ds(pl.multiple_of(side * half + first, LANES), ref.shape[1])
        copies.append(pltpu.make_async_copy(ref, out_ref.at[:, lanes], sems.at[at]))
    for copy in copies:
        copy.start()
    for copy in copies:
        copy.wait()


def place(pieces, base, shape, moves, name):
    vmem = pl.BlockSpec(memory_space=pltpu.VMEM)
    hbm = pl.BlockSpec(memory_space=pltpu.HBM)
    rest = () if base is None else (base,)
    return pl.pallas_call(
        partial(place_kernel, moves=moves),
        out_shape=jax.ShapeDtypeStruct(shape, jnp.bfloat16),
        in_specs=[vmem] * len(pieces) + [hbm] * len(rest),
        out_specs=hbm,
        scratch_shapes=[pltpu.SemaphoreType.DMA((len(moves),))],
        input_output_aliases={} if base is None else {len(pieces): 0},
        compiler_params=pltpu.CompilerParams(vmem_limit_bytes=VMEM_LIMIT),
        name=name,
    )(*pieces, *rest)


def places(frames, tile_rows, tile_cols, edge_rows):
    keys = []
    for at, (step, low, high) in enumerate(
        ((0, 0, tile_rows), (-1, tile_rows - edge_rows, tile_rows), (1, 0, edge_rows))
    ):
        shape = (frames, tile_cols, high - low)
        row = np.broadcast_to(np.arange(low, high), shape).reshape(-1)
        col = np.broadcast_to(np.arange(tile_cols)[:, None], shape).reshape(-1)
        for peer in (0, 1):
            keys.append(np.stack([row + step * tile_rows, row, col, 0 * row + 2 * at + peer]))
    query = np.concatenate(keys[:2], 1)[[0, 2, 3]]
    keys = np.concatenate(keys, 1)
    keys = np.concatenate([keys, 0 * keys]).astype(np.int32)
    query = np.concatenate([query, np.zeros((5, query.shape[1]))]).T.astype(np.int32)
    groups = np.arange(frames * tile_cols)[:, None] * tile_rows
    rows = np.arange(edge_rows)[None, :]
    chosen = np.concatenate(
        [(groups + tile_rows - edge_rows + rows).reshape(-1), (groups + rows).reshape(-1)]
    )
    select = (chosen[:, None] == np.arange(frames * tile_cols * tile_rows)[None, :]).astype(
        jnp.bfloat16
    )
    return keys, query, select


def swapped_body(queries, video_kv, text_kv, time_embed, gate_weight, window_extent, tile_valid):
    frames, tile_rows, tile_cols, model_width = queries.shape
    half = model_width // 2
    count = frames * tile_rows * tile_cols
    edge_rows = HALO + HALO % 2
    edge = frames * tile_cols * edge_rows
    near = 2 * count + 4 * edge
    text_count = text_kv.shape[1]
    text_rows = -(-text_count // LANES) * LANES
    tiles_down = lax.axis_size("th")
    swap = [(0, 1), (1, 0)]
    down = [(i, i + 1) for i in range(tiles_down - 1)]
    up = [(i + 1, i) for i in range(tiles_down - 1)]
    vmem = pl.BlockSpec(memory_space=pltpu.VMEM)
    smem = pl.BlockSpec(memory_space=pltpu.SMEM)
    params = pltpu.CompilerParams(vmem_limit_bytes=VMEM_LIMIT)
    key_places, query_places, select = places(frames, tile_rows, tile_cols, edge_rows)
    q = jnp.transpose(queries, (0, 2, 1, 3)).reshape(1, count, model_width)
    kv = jnp.transpose(video_kv, (0, 1, 3, 2, 4)).reshape(2, count, model_width)
    total_pairs = half // LANES
    pieces = []
    first = 0
    for share in CHUNKS:
        pairs = share * total_pairs // sum(CHUNKS)
        pieces.append((first, pairs))
        first += pairs
    head, tail = slice(0, 1), slice(1, 3)
    arrived = []
    for at, (first, pairs) in enumerate(pieces):
        low = first * LANES
        shapes = [(3, count, pairs * LANES)]
        moves = [(0, low, 0, head, True), (1, low, 0, tail, True)]
        last = at == len(pieces) - 1
        if last:
            shapes += [(1, count, half), (2, count, half)]
            moves += [(0, 0, 1, slice(0, 1), False), (1, 0, 2, slice(0, 2), False)]
        packed = pack(q, kv, shapes, tuple(moves), "pack")
        arrived.append(lax.ppermute(packed[0], "tw", swap))
        if last:
            mine_q, mine_kv = packed[1:]
    edge_shape = jax.ShapeDtypeStruct((2, edge, half), jnp.bfloat16)
    bottom, top, bias, gate, query_ok = pl.pallas_call(
        partial(prepare_kernel, tile_cols=tile_cols, tiles_down=tiles_down),
        out_shape=[
            edge_shape,
            edge_shape,
            jax.ShapeDtypeStruct((HALO * HALO, 2 * count, near), jnp.float32),
            jax.ShapeDtypeStruct((total_pairs, 1, LANES), jnp.float32),
            jax.ShapeDtypeStruct((2 * count, LANES), jnp.float32),
        ],
        in_specs=[smem] + [vmem] * 6,
        out_specs=[vmem] * 5,
        compiler_params=params,
        name="prepare",
    )(
        jnp.transpose(tile_valid.reshape(tiles_down, 2, 2), (1, 2, 0)),
        select,
        key_places,
        query_places,
        time_embed.reshape(1, -1),
        gate_weight,
        mine_kv,
    )
    above_mine = lax.ppermute(bottom, "th", down)
    below_mine = lax.ppermute(top, "th", up)
    text = jnp.pad(text_kv, ((0, 0), (0, text_rows - text_count), (0, 0)))
    extents = window_extent.T
    owned, returned = [], []
    for (first, pairs), peer in zip(pieces, arrived):
        width = pairs * LANES
        edge_shape = jax.ShapeDtypeStruct((2, edge, width), jnp.bfloat16)
        bottom, top = pl.pallas_call(
            edges_kernel,
            out_shape=[edge_shape] * 2,
            in_specs=[vmem] * 2 + [pl.BlockSpec(memory_space=pl.ANY)],
            out_specs=[vmem] * 2,
            compiler_params=params,
            name="edges",
        )(select, peer, text)
        above_peer = lax.ppermute(bottom, "th", down)
        below_peer = lax.ppermute(top, "th", up)
        unroll = math.gcd(pairs, UNROLL)
        own_out, peer_out = pl.pallas_call(
            partial(
                attend_kernel,
                first_pair=first,
                pairs=pairs,
                unroll=unroll,
                text_count=text_count,
                score_scale=HEAD_DIM ** (-0.5),
            ),
            out_shape=[jax.ShapeDtypeStruct((count, width), jnp.bfloat16)] * 2,
            in_specs=[smem] + [vmem] * 11,
            out_specs=[vmem] * 2,
            scratch_shapes=[pltpu.VMEM((unroll, near + text_rows, LANES), jnp.bfloat16)] * 2,
            compiler_params=params,
            name="attend",
        )(
            extents,
            mine_q,
            mine_kv,
            peer,
            above_mine,
            below_mine,
            above_peer,
            below_peer,
            text,
            bias,
            gate,
            query_ok,
        )
        owned.append(own_out)
        returned.append(lax.ppermute(peer_out, "tw", swap))
    starts = [first * LANES for first, _ in pieces]
    early = owned + returned[:-1]
    moves = [(i, low, False) for i, low in enumerate(starts)]
    moves += [(len(owned) + i, low, True) for i, low in enumerate(starts[:-1])]
    result = place(early, None, (count, model_width), tuple(moves), "place")
    moves = ((0, starts[-1], True),)
    result = place(returned[-1:], result, (count, model_width), moves, "place_last")
    result = result.reshape(frames, tile_cols, tile_rows, model_width)
    return jnp.transpose(result, (0, 2, 1, 3))


def solution(mesh):
    placed = (
        P("vid", "th", "tw", None),
        P(None, "vid", "th", "tw", None),
        P(None, "vid", "tw"),
        P("vid"),
        P(None, "tw"),
        P(),
        P("vid", None, None),
    )
    body = swapped_body if mesh.shape["tw"] == 2 else general_body
    return jax.shard_map(
        body, mesh=mesh, in_specs=placed, out_specs=P("vid", "th", "tw", None), check_vma=False
    )
```

```python
import math
from functools import partial

import jax
import jax.numpy as jnp
import numpy as np
from jax import lax
from jax.experimental import pallas as pl
from jax.experimental.pallas import tpu as pltpu
from jax.sharding import PartitionSpec as P


HEAD_DIM = 64
HALO = 3


NEG = -1e30


def extended(cells, sides, width):
    for axis, dim in sides:
        count = lax.axis_size(axis)
        ends = count - 1
        head = lax.slice_in_dim(cells, 0, width, axis=dim)
        tail = lax.slice_in_dim(cells, cells.shape[dim] - width, cells.shape[dim], axis=dim)
        cells = jnp.concatenate(
            [
                lax.ppermute(tail, axis, [(i, (i + 1) % count) for i in range(ends)]),
                cells,
                lax.ppermute(head, axis, [((i + 1) % count, i) for i in range(ends)]),
            ],
            axis=dim,
        )
    return cells


def key_validity(tile_valid, row_at, col_at, tile_rows, tile_cols):
    tiles_down = tile_valid.shape[0]
    tiles_across = tile_valid.shape[1]
    glob_row = row_at * tile_rows + jnp.arange(tile_rows + 2 * HALO, dtype=jnp.int32) - HALO
    glob_col = col_at * tile_cols + jnp.arange(tile_cols + 2 * HALO, dtype=jnp.int32) - HALO
    tile_row = jnp.floor_divide(glob_row, tile_rows)
    tile_col = jnp.floor_divide(glob_col, tile_cols)
    pick_row = (tile_row[:, None] == jnp.arange(tiles_down, dtype=jnp.int32)[None, :]).astype(
        jnp.float32
    )
    pick_col = (tile_col[:, None] == jnp.arange(tiles_across, dtype=jnp.int32)[None, :]).astype(
        jnp.float32
    )
    table = tile_valid.astype(jnp.float32)
    high = lax.Precision.HIGHEST
    limit_rows = jnp.dot(
        jnp.dot(pick_row, table[..., 0], precision=high), pick_col.T, precision=high
    )
    limit_cols = jnp.dot(
        jnp.dot(pick_row, table[..., 1], precision=high), pick_col.T, precision=high
    )
    local_row = (glob_row - tile_row * tile_rows).astype(jnp.float32)
    local_col = (glob_col - tile_col * tile_cols).astype(jnp.float32)
    return (local_row[:, None] < limit_rows) & (local_col[None, :] < limit_cols)


def video_part(
    query_rows,
    video_keys,
    video_values,
    key_ok,
    window_extent,
    frames,
    tile_rows,
    tile_cols,
    score_scale,
):
    count_q, head_count, head_depth = query_rows.shape
    count_k = video_keys.shape[0]
    span_rows = tile_rows + 2 * HALO
    span_cols = tile_cols + 2 * HALO
    per_turn = math.gcd(head_count, 4)
    query_ids = jnp.arange(count_q, dtype=jnp.int32)
    key_ids = jnp.arange(count_k, dtype=jnp.int32)
    query_row = query_ids // tile_cols % tile_rows
    query_col = query_ids % tile_cols
    key_row = key_ids // span_cols % span_rows
    key_col = key_ids % span_cols
    row_gap = jnp.abs(key_row[None, :] - query_row[:, None] - HALO)
    col_gap = jnp.abs(key_col[None, :] - query_col[:, None] - HALO)
    key_flat = jnp.tile(key_ok.reshape(-1), frames)

    def one_group(turn_index, carry):
        video_out, video_max, video_total = carry
        first_head = jnp.asarray(turn_index, jnp.int32) * per_turn
        query_part = lax.dynamic_slice_in_dim(query_rows, first_head, per_turn, 1)
        key_part = lax.dynamic_slice_in_dim(video_keys, first_head, per_turn, 1)
        value_part = lax.dynamic_slice_in_dim(video_values, first_head, per_turn, 1)
        extents = lax.dynamic_slice_in_dim(window_extent, first_head, per_turn, 0)
        allowed = (
            (row_gap[None] <= extents[:, 0][:, None, None])
            & (col_gap[None] <= extents[:, 1][:, None, None])
            & key_flat[None, None, :]
        )
        scores = (
            jnp.einsum("nhd,khd->hnk", query_part, key_part, preferred_element_type=jnp.float32)
            * score_scale
        )
        scores = jnp.where(allowed, scores, NEG)
        maximum = jnp.max(scores, axis=-1)
        exp_terms = jnp.where(allowed, jnp.exp(scores - maximum[..., None]), 0.0)
        totals = jnp.sum(exp_terms, axis=-1)
        weights = exp_terms.astype(jnp.bfloat16)
        partial_value = jnp.einsum(
            "hnk,khd->nhd", weights, value_part, preferred_element_type=jnp.float32
        )
        video_out = lax.dynamic_update_slice_in_dim(video_out, partial_value, first_head, 1)
        video_max = lax.dynamic_update_slice_in_dim(video_max, maximum, first_head, 0)
        video_total = lax.dynamic_update_slice_in_dim(video_total, totals, first_head, 0)
        return (video_out, video_max, video_total)

    initial = (
        jnp.zeros((count_q, head_count, head_depth), jnp.float32),
        jnp.zeros((head_count, count_q), jnp.float32),
        jnp.zeros((head_count, count_q), jnp.float32),
    )
    return lax.fori_loop(0, head_count // per_turn, one_group, initial)


def text_part(query_rows, text_keys, text_values, score_scale):
    scores = (
        jnp.einsum("nhd,thd->nht", query_rows, text_keys, preferred_element_type=jnp.float32)
        * score_scale
    )
    maximum = jnp.max(scores, axis=-1)
    exp_terms = jnp.exp(scores - maximum[..., None])
    totals = jnp.sum(exp_terms, axis=-1)
    partial_value = jnp.einsum(
        "nht,thd->nhd",
        exp_terms.astype(jnp.bfloat16),
        text_values,
        preferred_element_type=jnp.float32,
    )
    return (partial_value, maximum, totals)


def combine(video_out, video_max, video_total, text_out, text_max, text_total):
    max_v = video_max.T
    total_v = video_total.T
    joint_max = jnp.maximum(max_v, text_max)
    scale_v = jnp.exp(max_v - joint_max)
    scale_t = jnp.exp(text_max - joint_max)
    denom = total_v * scale_v + text_total * scale_t
    return (video_out * scale_v[..., None] + text_out * scale_t[..., None]) / denom[..., None]


def attend_tile(
    query_block,
    kv_block,
    text_keys,
    text_values,
    extents,
    gate_vec,
    key_ok,
    tile_rows,
    tile_cols,
    score_scale,
):
    frames = query_block.shape[0]
    width = query_block.shape[3]
    head_count = width // HEAD_DIM
    query_rows = query_block.reshape(-1, head_count, HEAD_DIM)
    video_keys = kv_block[0].reshape(-1, head_count, HEAD_DIM)
    video_values = kv_block[1].reshape(-1, head_count, HEAD_DIM)
    video_out, video_max, video_total = video_part(
        query_rows,
        video_keys,
        video_values,
        key_ok,
        extents,
        frames,
        tile_rows,
        tile_cols,
        score_scale,
    )
    text_out, text_max, text_total = text_part(query_rows, text_keys, text_values, score_scale)
    attended = combine(video_out, video_max, video_total, text_out, text_max, text_total)
    attended = attended.reshape(frames, tile_rows, tile_cols, width)
    query_ok = key_ok[HALO : HALO + tile_rows, HALO : HALO + tile_cols]
    result = jnp.where(query_ok[None, :, :, None], gate_vec.astype(jnp.float32) * attended, 0.0)
    return result.astype(jnp.bfloat16)


def general_body(queries, video_kv, text_kv, time_embed, gate_weight, window_extent, tile_valid):
    _, tile_rows, tile_cols, model_width = queries.shape
    head_count = model_width // HEAD_DIM
    score_scale = HEAD_DIM ** (-0.5)
    text_count = text_kv.shape[1]
    row_at = lax.axis_index("th")
    col_at = lax.axis_index("tw")
    mod_in = jax.nn.silu(time_embed.astype(jnp.float32)).astype(jnp.bfloat16)
    gate_part = jnp.dot(mod_in[None, :], gate_weight, preferred_element_type=jnp.float32)[0].astype(
        jnp.bfloat16
    )
    padded = extended(video_kv, (("th", 2), ("tw", 3)), HALO)
    text_full, gate_full = (
        lax.all_gather(text_kv, "tw", axis=2, tiled=True),
        lax.all_gather(gate_part, "tw", axis=0, tiled=True),
    )
    text_keys = text_full[0].reshape(text_count, head_count, HEAD_DIM)
    text_values = text_full[1].reshape(text_count, head_count, HEAD_DIM)
    key_ok = key_validity(tile_valid, row_at, col_at, tile_rows, tile_cols)
    return attend_tile(
        queries,
        padded,
        text_keys,
        text_values,
        window_extent,
        gate_full,
        key_ok,
        tile_rows,
        tile_cols,
        score_scale,
    )


LANES = 128
CHUNKS = (7, 5)
UNROLL = 4
VMEM_LIMIT = 16 * 2**20


def pack_kernel(q_ref, kv_ref, *refs, moves):
    outs, sems = refs[:-1], refs[-1]
    col_at = lax.axis_index("tw")
    half = q_ref.shape[2] // 2
    copies = []
    for at, (source, first, out, slot, other) in enumerate(moves):
        to = outs[out].at[slot]
        side = 1 - col_at if other else col_at
        lanes = pl.ds(pl.multiple_of(side * half + first, LANES), to.shape[2])
        ref = q_ref if source == 0 else kv_ref
        copies.append(pltpu.make_async_copy(ref.at[:, :, lanes], to, sems.at[at]))
    for copy in copies:
        copy.start()
    for copy in copies:
        copy.wait()


def pack(q, kv, shapes, moves):
    return pl.pallas_call(
        partial(pack_kernel, moves=moves),
        out_shape=[jax.ShapeDtypeStruct(shape, q.dtype) for shape in shapes],
        in_specs=[pl.BlockSpec(memory_space=pltpu.HBM)] * 2,
        out_specs=[pl.BlockSpec(memory_space=pltpu.VMEM)] * len(shapes),
        scratch_shapes=[pltpu.SemaphoreType.DMA((len(moves),))],
        compiler_params=pltpu.CompilerParams(vmem_limit_bytes=VMEM_LIMIT),
    )(q, kv)


def cut_edges(select_ref, keys_values, bottom_ref, top_ref):
    edge = bottom_ref.shape[1]
    for part in (0, 1):
        rows = lax.dot_general(
            select_ref[...],
            keys_values[part],
            (((1,), (0,)), ((), ())),
            preferred_element_type=jnp.float32,
        ).astype(jnp.bfloat16)
        bottom_ref[part] = rows[:edge]
        top_ref[part] = rows[edge:]


def edges_kernel(select_ref, peer_ref, *refs):
    cut_edges(select_ref, (peer_ref[1], peer_ref[2]), *refs[-2:])


def own_edges_kernel(select_ref, mine_ref, other_ref, bottom_ref, top_ref):
    half = mine_ref.shape[2]
    for ref, skip, low, high in (
        (mine_ref, 0, 0, half),
        (other_ref, 1, half, bottom_ref.shape[2]),
    ):
        cut_edges(
            select_ref,
            (ref[skip], ref[skip + 1]),
            bottom_ref.at[:, :, low:high],
            top_ref.at[:, :, low:high],
        )


def join_kernel(above_ref, below_ref, out_ref):
    edge = above_ref.shape[1]
    skip = above_ref.shape[2] - out_ref.shape[2]
    for part in (0, 1):
        out_ref[part, :edge] = above_ref[part, :, skip:]
        out_ref[part, edge:] = below_ref[part, :, skip:]


def prepare_kernel(
    valid_ref,
    key_ref,
    query_ref,
    time_ref,
    weight_ref,
    bias_ref,
    gate_ref,
    ok_ref,
    *,
    tile_cols,
    tiles_down,
):
    row_at = lax.axis_index("th")
    col_at = lax.axis_index("tw")
    key_row, key_local, key_col, key_block = (key_ref[i : i + 1] for i in range(4))
    query_row, query_col, query_peer = (query_ref[:, i : i + 1] for i in range(3))
    key_peer = key_block % 2
    row_limit = jnp.zeros_like(key_row)
    col_limit = jnp.zeros_like(key_row)
    query_limits = []
    for at, step in enumerate((0, -1, 1)):
        tile_row = row_at + step
        inside = (tile_row >= 0) & (tile_row < tiles_down)
        tile_row = jnp.clip(tile_row, 0, tiles_down - 1)
        for peer in (0, 1):
            side = 1 - col_at if peer else col_at
            rows = jnp.where(inside, valid_ref[side, 0, tile_row], 0)
            cols = valid_ref[side, 1, tile_row]
            block = 2 * at + peer
            row_limit = jnp.where(key_block == block, rows, row_limit)
            col_limit = jnp.where(key_block == block, cols, col_limit)
            if step == 0:
                query_limits.append((rows, cols))
    key_ok = (key_local < row_limit) & (key_col < col_limit)
    key_at = key_col + tile_cols * jnp.where(key_peer > 0, 1 - col_at, col_at)
    query_at = query_col + tile_cols * jnp.where(query_peer > 0, 1 - col_at, col_at)
    row_gap = jnp.abs(query_row - key_row)
    col_gap = jnp.where(key_ok, jnp.abs(query_at - key_at), 2 * HALO + 1)
    for rows in range(HALO):
        for cols in range(HALO):
            near = (row_gap <= rows + 1) & (col_gap <= cols + 1)
            bias_ref[rows * HALO + cols] = jnp.where(near, 0.0, NEG)
    row_limit = jnp.where(query_peer > 0, query_limits[1][0], query_limits[0][0])
    col_limit = jnp.where(query_peer > 0, query_limits[1][1], query_limits[0][1])
    query_ok = (query_row < row_limit) & (query_col < col_limit)
    ok_ref[...] = jnp.broadcast_to(jnp.where(query_ok, 1.0, 0.0), ok_ref.shape)
    step = time_ref[...].astype(jnp.float32)
    step = (step / (1.0 + jnp.exp(-step))).astype(jnp.bfloat16)
    gate = jnp.dot(step, weight_ref[...], preferred_element_type=jnp.float32)
    gate = gate.astype(jnp.bfloat16).astype(jnp.float32)
    for pair in range(gate_ref.shape[0]):
        gate_ref[pair] = gate[0:1, pair * LANES : (pair + 1) * LANES]


def attend_kernel(
    extent_ref,
    mine_q_ref,
    mine_kv_ref,
    peer_ref,
    above_mine_ref,
    below_mine_ref,
    text_ref,
    bias_ref,
    gate_ref,
    ok_ref,
    *refs,
    first_pair,
    pairs,
    unroll,
    text_count,
    score_scale,
):
    *edges, own_out_ref, peer_out_ref, key_ref, value_ref = refs
    above_peer, below_peer = edges[0], edges[-1]
    count = mine_q_ref.shape[1]
    edge = above_mine_ref.shape[1]
    near = 2 * count + 4 * edge
    first_head = lax.axis_index("tw") * (2 * gate_ref.shape[0])
    left = lax.broadcasted_iota(jnp.int32, (1, LANES), 1) < HEAD_DIM
    zero = jnp.zeros((), jnp.bfloat16)
    text_rows = text_ref.shape[1]
    text_bias = jnp.where(
        lax.broadcasted_iota(jnp.int32, (1, text_rows), 1) < text_count, 0.0, NEG
    )

    def lanes_of(turn):
        start = turn * LANES
        if not isinstance(start, int):
            start = pl.multiple_of(start, LANES)
        return pl.ds(start, LANES)

    def score(turn, slot):
        here, whole = lanes_of(turn), lanes_of(first_pair + turn)
        for part, into in ((0, key_ref.at[slot]), (1, value_ref.at[slot])):
            into[0:count] = mine_kv_ref[part, :, whole]
            into[count : 2 * count] = peer_ref[1 + part, :, here]
            at = 2 * count
            for ref, low, lanes in (
                (above_mine_ref, 0, whole),
                (above_peer, 0, here),
                (below_mine_ref, 0, whole),
                (below_peer, below_peer.shape[1] - edge, here),
            ):
                into[at : at + edge] = ref[part, low : low + edge, lanes]
                at += edge
            into[near:] = text_ref[part, :, whole]
        queries = jnp.concatenate([mine_q_ref[0, :, whole], peer_ref[0, :, here]], 0)
        queries = queries * jnp.asarray(score_scale, jnp.bfloat16)
        queries = jnp.concatenate([jnp.where(left, queries, zero), jnp.where(left, zero, queries)], 0)
        return lax.dot_general(
            queries, key_ref[slot], (((1,), (1,)), ((), ())), preferred_element_type=jnp.float32
        )

    def mix(turn, slot, both):
        here = lanes_of(turn)
        weights, shares = [], []
        for side in (0, 1):
            head = first_head + 2 * (first_pair + turn) + side
            reach_rows = jnp.clip(extent_ref[0, head], 1, HALO) - 1
            reach_cols = jnp.clip(extent_ref[1, head], 1, HALO) - 1
            bias = bias_ref[reach_rows * HALO + reach_cols]
            scores = both[2 * count * side : 2 * count * (side + 1)]
            scores = jnp.concatenate([scores[:, :near] + bias, scores[:, near:] + text_bias], 1)
            terms = jnp.exp(scores - jnp.max(scores, axis=-1, keepdims=True))
            shares.append(1.0 / jnp.sum(terms, axis=-1, keepdims=True))
            weights.append(terms.astype(jnp.bfloat16))
        sums = lax.dot_general(
            jnp.concatenate(weights, 0),
            value_ref[slot],
            (((1,), (0,)), ((), ())),
            preferred_element_type=jnp.float32,
        )
        attended = jnp.where(left, sums[: 2 * count] * shares[0], sums[2 * count :] * shares[1])
        gated = jnp.where(ok_ref[...] > 0.0, attended * gate_ref[first_pair + turn], 0.0)
        gated = gated.astype(jnp.bfloat16)
        own_out_ref[:, here] = gated[:count]
        peer_out_ref[:, here] = gated[count:]

    def some_pairs(first, size):
        turns = [(first + slot, slot) for slot in range(size)]
        scored = [score(*turn) for turn in turns]
        for turn, both in zip(turns, scored):
            mix(*turn, both)

    steps = -(-pairs // unroll)
    low, extra = divmod(pairs, steps)
    if extra:
        at = 0
        for step in range(steps):
            some_pairs(at, low + (step < extra))
            at += low + (step < extra)
    else:
        lax.fori_loop(0, steps, lambda step, _: some_pairs(step * low, low), None)


def place_kernel(*refs, moves):
    ins, out_ref, sems = refs[:-2], refs[-2], refs[-1]
    col_at = lax.axis_index("tw")
    half = out_ref.shape[1] // 2
    copies = []
    for at, (source, first, other) in enumerate(moves):
        side = 1 - col_at if other else col_at
        ref = ins[source]
        lanes = pl.ds(pl.multiple_of(side * half + first, LANES), ref.shape[1])
        copies.append(pltpu.make_async_copy(ref, out_ref.at[:, lanes], sems.at[at]))
    for copy in copies:
        copy.start()
    for copy in copies:
        copy.wait()


def place(pieces, base, shape, moves):
    vmem = pl.BlockSpec(memory_space=pltpu.VMEM)
    hbm = pl.BlockSpec(memory_space=pltpu.HBM)
    rest = () if base is None else (base,)
    return pl.pallas_call(
        partial(place_kernel, moves=moves),
        out_shape=jax.ShapeDtypeStruct(shape, jnp.bfloat16),
        in_specs=[vmem] * len(pieces) + [hbm] * len(rest),
        out_specs=hbm,
        scratch_shapes=[pltpu.SemaphoreType.DMA((len(moves),))],
        input_output_aliases={} if base is None else {len(pieces): 0},
        compiler_params=pltpu.CompilerParams(vmem_limit_bytes=VMEM_LIMIT),
    )(*pieces, *rest)


def places(frames, tile_rows, tile_cols, edge_rows):
    keys = []
    for at, (step, low, high) in enumerate(
        ((0, 0, tile_rows), (-1, tile_rows - edge_rows, tile_rows), (1, 0, edge_rows))
    ):
        shape = (frames, tile_cols, high - low)
        row = np.broadcast_to(np.arange(low, high), shape).reshape(-1)
        col = np.broadcast_to(np.arange(tile_cols)[:, None], shape).reshape(-1)
        for peer in (0, 1):
            keys.append(np.stack([row + step * tile_rows, row, col, 0 * row + 2 * at + peer]))
    query = np.concatenate(keys[:2], 1)[[0, 2, 3]]
    keys = np.concatenate(keys, 1)
    keys = np.concatenate([keys, 0 * keys]).astype(np.int32)
    query = np.concatenate([query, np.zeros((5, query.shape[1]))]).T.astype(np.int32)
    groups = np.arange(frames * tile_cols)[:, None] * tile_rows
    rows = np.arange(edge_rows)[None, :]
    chosen = np.concatenate(
        [(groups + tile_rows - edge_rows + rows).reshape(-1), (groups + rows).reshape(-1)]
    )
    select = (chosen[:, None] == np.arange(frames * tile_cols * tile_rows)[None, :]).astype(
        jnp.bfloat16
    )
    return keys, query, select


def swapped_body(queries, video_kv, text_kv, time_embed, gate_weight, window_extent, tile_valid):
    frames, tile_rows, tile_cols, model_width = queries.shape
    half = model_width // 2
    count = frames * tile_rows * tile_cols
    edge_rows = HALO + HALO % 2
    edge = frames * tile_cols * edge_rows
    near = 2 * count + 4 * edge
    text_count = text_kv.shape[1]
    text_rows = -(-text_count // LANES) * LANES
    tiles_down = lax.axis_size("th")
    swap = [(0, 1), (1, 0)]
    down = [(i, i + 1) for i in range(tiles_down - 1)]
    up = [(i + 1, i) for i in range(tiles_down - 1)]
    vmem = pl.BlockSpec(memory_space=pltpu.VMEM)
    smem = pl.BlockSpec(memory_space=pltpu.SMEM)
    params = pltpu.CompilerParams(vmem_limit_bytes=VMEM_LIMIT)
    key_places, query_places, select = places(frames, tile_rows, tile_cols, edge_rows)
    q = jnp.transpose(queries, (0, 2, 1, 3)).reshape(1, count, model_width)
    kv = jnp.transpose(video_kv, (0, 1, 3, 2, 4)).reshape(2, count, model_width)
    q = pltpu.with_memory_space_constraint(q, pltpu.HBM)
    kv = pltpu.with_memory_space_constraint(kv, pltpu.HBM)
    total_pairs = half // LANES
    pieces = []
    first = 0
    for share in CHUNKS:
        pairs = share * total_pairs // sum(CHUNKS)
        pieces.append((first, pairs))
        first += pairs
    head, tail = slice(0, 1), slice(1, 3)
    (first, pairs), (last, rest) = pieces
    low, width, end = first * LANES, pairs * LANES, rest * LANES
    moves = ((0, low, 0, head, True), (1, low, 0, tail, True))
    (sent,) = pack(q, kv, [(3, count, width)], moves)
    arrived = [lax.ppermute(sent, "tw", swap)]
    shapes = [(3, count, end), (1, count, half), (2, count, half)]
    low = last * LANES
    moves = (
        (0, 0, 1, slice(0, 1), False),
        (1, 0, 2, slice(0, 2), False),
        (0, low, 0, head, True),
        (1, low, 0, tail, True),
    )
    sent, mine_q, mine_kv = pack(q, kv, shapes, moves)
    bottom, top = pl.pallas_call(
        own_edges_kernel,
        out_shape=[jax.ShapeDtypeStruct((2, edge, half + end), jnp.bfloat16)] * 2,
        in_specs=[vmem] * 3,
        out_specs=[vmem] * 2,
        compiler_params=params,
        name="own_edges",
    )(select, mine_kv, sent)
    above_mine = lax.ppermute(bottom, "th", down)
    below_mine = lax.ppermute(top, "th", up)
    arrived.append(lax.ppermute(sent, "tw", swap))
    joined = pl.pallas_call(
        join_kernel,
        out_shape=jax.ShapeDtypeStruct((2, 2 * edge, end), jnp.bfloat16),
        in_specs=[vmem] * 2,
        out_specs=vmem,
        compiler_params=params,
        name="join",
    )(above_mine, below_mine)
    joined = lax.ppermute(joined, "tw", swap)
    bias, gate, query_ok = pl.pallas_call(
        partial(prepare_kernel, tile_cols=tile_cols, tiles_down=tiles_down),
        out_shape=[
            jax.ShapeDtypeStruct((HALO * HALO, 2 * count, near), jnp.float32),
            jax.ShapeDtypeStruct((total_pairs, 1, LANES), jnp.float32),
            jax.ShapeDtypeStruct((2 * count, LANES), jnp.float32),
        ],
        in_specs=[smem] + [vmem] * 4,
        out_specs=[vmem] * 3,
        compiler_params=params,
        name="prepare",
    )(
        jnp.transpose(tile_valid.reshape(tiles_down, 2, 2), (1, 2, 0)),
        key_places,
        query_places,
        time_embed.reshape(1, -1),
        gate_weight,
    )
    text = jnp.pad(text_kv, ((0, 0), (0, text_rows - text_count), (0, 0)))
    extents = window_extent.T
    owned, returned = [], []
    for at, ((first, pairs), peer) in enumerate(zip(pieces, arrived)):
        width = pairs * LANES
        edges = (joined,)
        if at == 0:
            bottom, top = pl.pallas_call(
                edges_kernel,
                out_shape=[jax.ShapeDtypeStruct((2, edge, width), jnp.bfloat16)] * 2,
                in_specs=[vmem] * 2 + [pl.BlockSpec(memory_space=pl.ANY)],
                out_specs=[vmem] * 2,
                compiler_params=params,
                name="edges",
            )(select, peer, text)
            above_peer = lax.ppermute(bottom, "th", down)
            below_peer = lax.ppermute(top, "th", up)
            edges = (above_peer, below_peer)
        unroll = min(pairs, UNROLL)
        own_out, peer_out = pl.pallas_call(
            partial(
                attend_kernel,
                first_pair=first,
                pairs=pairs,
                unroll=unroll,
                text_count=text_count,
                score_scale=HEAD_DIM ** (-0.5),
            ),
            out_shape=[jax.ShapeDtypeStruct((count, width), jnp.bfloat16)] * 2,
            in_specs=[smem] + [vmem] * (9 + len(edges)),
            out_specs=[vmem] * 2,
            scratch_shapes=[pltpu.VMEM((unroll, near + text_rows, LANES), jnp.bfloat16)] * 2,
            compiler_params=params,
        )(
            extents,
            mine_q,
            mine_kv,
            peer,
            above_mine,
            below_mine,
            text,
            bias,
            gate,
            query_ok,
            *edges,
        )
        owned.append(own_out)
        returned.append(lax.ppermute(peer_out, "tw", swap))
    starts = [first * LANES for first, _ in pieces]
    early = owned + returned[:-1]
    moves = [(i, low, False) for i, low in enumerate(starts)]
    moves += [(len(owned) + i, low, True) for i, low in enumerate(starts[:-1])]
    result = place(early, None, (count, model_width), tuple(moves))
    moves = ((0, starts[-1], True),)
    result = place(returned[-1:], result, (count, model_width), moves)
    result = result.reshape(frames, tile_cols, tile_rows, model_width)
    return jnp.transpose(result, (0, 2, 1, 3))


def solution(mesh):
    placed = (
        P("vid", "th", "tw", None),
        P(None, "vid", "th", "tw", None),
        P(None, "vid", "tw"),
        P("vid"),
        P(None, "tw"),
        P(),
        P("vid", None, None),
    )
    swapped = mesh.shape["tw"] == 2
    body = swapped_body if swapped else general_body

    return jax.shard_map(
        body, mesh=mesh, in_specs=placed, out_specs=P("vid", "th", "tw", None), check_vma=False
    )
```

```python
import math
from functools import partial

import jax
import jax.numpy as jnp
import numpy as np
from jax import lax
from jax.experimental import pallas as pl
from jax.experimental.pallas import tpu as pltpu
from jax.sharding import PartitionSpec as P


HEAD_DIM = 64
HALO = 3


NEG = -1e30


def extended(cells, sides, width):
    for axis, dim in sides:
        count = lax.axis_size(axis)
        ends = count - 1
        head = lax.slice_in_dim(cells, 0, width, axis=dim)
        tail = lax.slice_in_dim(cells, cells.shape[dim] - width, cells.shape[dim], axis=dim)
        cells = jnp.concatenate(
            [
                lax.ppermute(tail, axis, [(i, (i + 1) % count) for i in range(ends)]),
                cells,
                lax.ppermute(head, axis, [((i + 1) % count, i) for i in range(ends)]),
            ],
            axis=dim,
        )
    return cells


def key_validity(tile_valid, row_at, col_at, tile_rows, tile_cols):
    tiles_down = tile_valid.shape[0]
    tiles_across = tile_valid.shape[1]
    glob_row = row_at * tile_rows + jnp.arange(tile_rows + 2 * HALO, dtype=jnp.int32) - HALO
    glob_col = col_at * tile_cols + jnp.arange(tile_cols + 2 * HALO, dtype=jnp.int32) - HALO
    tile_row = jnp.floor_divide(glob_row, tile_rows)
    tile_col = jnp.floor_divide(glob_col, tile_cols)
    pick_row = (tile_row[:, None] == jnp.arange(tiles_down, dtype=jnp.int32)[None, :]).astype(
        jnp.float32
    )
    pick_col = (tile_col[:, None] == jnp.arange(tiles_across, dtype=jnp.int32)[None, :]).astype(
        jnp.float32
    )
    table = tile_valid.astype(jnp.float32)
    high = lax.Precision.HIGHEST
    limit_rows = jnp.dot(
        jnp.dot(pick_row, table[..., 0], precision=high), pick_col.T, precision=high
    )
    limit_cols = jnp.dot(
        jnp.dot(pick_row, table[..., 1], precision=high), pick_col.T, precision=high
    )
    local_row = (glob_row - tile_row * tile_rows).astype(jnp.float32)
    local_col = (glob_col - tile_col * tile_cols).astype(jnp.float32)
    return (local_row[:, None] < limit_rows) & (local_col[None, :] < limit_cols)


def video_part(
    query_rows,
    video_keys,
    video_values,
    key_ok,
    window_extent,
    frames,
    tile_rows,
    tile_cols,
    score_scale,
):
    count_q, head_count, head_depth = query_rows.shape
    count_k = video_keys.shape[0]
    span_rows = tile_rows + 2 * HALO
    span_cols = tile_cols + 2 * HALO
    per_turn = math.gcd(head_count, 4)
    query_ids = jnp.arange(count_q, dtype=jnp.int32)
    key_ids = jnp.arange(count_k, dtype=jnp.int32)
    query_row = query_ids // tile_cols % tile_rows
    query_col = query_ids % tile_cols
    key_row = key_ids // span_cols % span_rows
    key_col = key_ids % span_cols
    row_gap = jnp.abs(key_row[None, :] - query_row[:, None] - HALO)
    col_gap = jnp.abs(key_col[None, :] - query_col[:, None] - HALO)
    key_flat = jnp.tile(key_ok.reshape(-1), frames)

    def one_group(turn_index, carry):
        video_out, video_max, video_total = carry
        first_head = jnp.asarray(turn_index, jnp.int32) * per_turn
        query_part = lax.dynamic_slice_in_dim(query_rows, first_head, per_turn, 1)
        key_part = lax.dynamic_slice_in_dim(video_keys, first_head, per_turn, 1)
        value_part = lax.dynamic_slice_in_dim(video_values, first_head, per_turn, 1)
        extents = lax.dynamic_slice_in_dim(window_extent, first_head, per_turn, 0)
        allowed = (
            (row_gap[None] <= extents[:, 0][:, None, None])
            & (col_gap[None] <= extents[:, 1][:, None, None])
            & key_flat[None, None, :]
        )
        scores = (
            jnp.einsum("nhd,khd->hnk", query_part, key_part, preferred_element_type=jnp.float32)
            * score_scale
        )
        scores = jnp.where(allowed, scores, NEG)
        maximum = jnp.max(scores, axis=-1)
        exp_terms = jnp.where(allowed, jnp.exp(scores - maximum[..., None]), 0.0)
        totals = jnp.sum(exp_terms, axis=-1)
        weights = exp_terms.astype(jnp.bfloat16)
        partial_value = jnp.einsum(
            "hnk,khd->nhd", weights, value_part, preferred_element_type=jnp.float32
        )
        video_out = lax.dynamic_update_slice_in_dim(video_out, partial_value, first_head, 1)
        video_max = lax.dynamic_update_slice_in_dim(video_max, maximum, first_head, 0)
        video_total = lax.dynamic_update_slice_in_dim(video_total, totals, first_head, 0)
        return (video_out, video_max, video_total)

    initial = (
        jnp.zeros((count_q, head_count, head_depth), jnp.float32),
        jnp.zeros((head_count, count_q), jnp.float32),
        jnp.zeros((head_count, count_q), jnp.float32),
    )
    return lax.fori_loop(0, head_count // per_turn, one_group, initial)


def text_part(query_rows, text_keys, text_values, score_scale):
    scores = (
        jnp.einsum("nhd,thd->nht", query_rows, text_keys, preferred_element_type=jnp.float32)
        * score_scale
    )
    maximum = jnp.max(scores, axis=-1)
    exp_terms = jnp.exp(scores - maximum[..., None])
    totals = jnp.sum(exp_terms, axis=-1)
    partial_value = jnp.einsum(
        "nht,thd->nhd",
        exp_terms.astype(jnp.bfloat16),
        text_values,
        preferred_element_type=jnp.float32,
    )
    return (partial_value, maximum, totals)


def combine(video_out, video_max, video_total, text_out, text_max, text_total):
    max_v = video_max.T
    total_v = video_total.T
    joint_max = jnp.maximum(max_v, text_max)
    scale_v = jnp.exp(max_v - joint_max)
    scale_t = jnp.exp(text_max - joint_max)
    denom = total_v * scale_v + text_total * scale_t
    return (video_out * scale_v[..., None] + text_out * scale_t[..., None]) / denom[..., None]


def attend_tile(
    query_block,
    kv_block,
    text_keys,
    text_values,
    extents,
    gate_vec,
    key_ok,
    tile_rows,
    tile_cols,
    score_scale,
):
    frames = query_block.shape[0]
    width = query_block.shape[3]
    head_count = width // HEAD_DIM
    query_rows = query_block.reshape(-1, head_count, HEAD_DIM)
    video_keys = kv_block[0].reshape(-1, head_count, HEAD_DIM)
    video_values = kv_block[1].reshape(-1, head_count, HEAD_DIM)
    video_out, video_max, video_total = video_part(
        query_rows,
        video_keys,
        video_values,
        key_ok,
        extents,
        frames,
        tile_rows,
        tile_cols,
        score_scale,
    )
    text_out, text_max, text_total = text_part(query_rows, text_keys, text_values, score_scale)
    attended = combine(video_out, video_max, video_total, text_out, text_max, text_total)
    attended = attended.reshape(frames, tile_rows, tile_cols, width)
    query_ok = key_ok[HALO : HALO + tile_rows, HALO : HALO + tile_cols]
    result = jnp.where(query_ok[None, :, :, None], gate_vec.astype(jnp.float32) * attended, 0.0)
    return result.astype(jnp.bfloat16)


def general_body(queries, video_kv, text_kv, time_embed, gate_weight, window_extent, tile_valid):
    _, tile_rows, tile_cols, model_width = queries.shape
    head_count = model_width // HEAD_DIM
    score_scale = HEAD_DIM ** (-0.5)
    text_count = text_kv.shape[1]
    row_at = lax.axis_index("th")
    col_at = lax.axis_index("tw")
    mod_in = jax.nn.silu(time_embed.astype(jnp.float32)).astype(jnp.bfloat16)
    gate_part = jnp.dot(mod_in[None, :], gate_weight, preferred_element_type=jnp.float32)[0].astype(
        jnp.bfloat16
    )
    padded = extended(video_kv, (("th", 2), ("tw", 3)), HALO)
    text_full, gate_full = (
        lax.all_gather(text_kv, "tw", axis=2, tiled=True),
        lax.all_gather(gate_part, "tw", axis=0, tiled=True),
    )
    text_keys = text_full[0].reshape(text_count, head_count, HEAD_DIM)
    text_values = text_full[1].reshape(text_count, head_count, HEAD_DIM)
    key_ok = key_validity(tile_valid, row_at, col_at, tile_rows, tile_cols)
    return attend_tile(
        queries,
        padded,
        text_keys,
        text_values,
        window_extent,
        gate_full,
        key_ok,
        tile_rows,
        tile_cols,
        score_scale,
    )


LANES = 128
CHUNKS = (7, 5)
UNROLL = 4
TEXT_BLOCK = 6
VMEM_LIMIT = 16 * 2**20


def pack_kernel(q_ref, kv_ref, *refs, moves):
    outs, sems = refs[:-1], refs[-1]
    col_at = lax.axis_index("tw")
    half = q_ref.shape[2] // 2
    copies = []
    for source, first, out, slot, other in moves:
        to = outs[out].at[slot]
        side = 1 - col_at if other else col_at
        lanes = pl.ds(pl.multiple_of(side * half + first, LANES), to.shape[2])
        ref = q_ref if source == 0 else kv_ref
        copies.append(pltpu.make_async_copy(ref.at[:, :, lanes], to, sems.at[len(copies)]))
    for copy in copies:
        copy.start()
    for copy in copies:
        copy.wait()


def pack(q, kv, shapes, moves):
    return pl.pallas_call(
        partial(pack_kernel, moves=moves),
        out_shape=[jax.ShapeDtypeStruct(shape, q.dtype) for shape in shapes],
        in_specs=[pl.BlockSpec(memory_space=pltpu.HBM)] * 2,
        out_specs=[pl.BlockSpec(memory_space=pltpu.VMEM)] * len(shapes),
        scratch_shapes=[pltpu.SemaphoreType.DMA((len(moves),))],
        compiler_params=pltpu.CompilerParams(vmem_limit_bytes=VMEM_LIMIT),
    )(q, kv)


def cut_edges(select, keys_values, *outs):
    for part in (0, 1):
        rows = lax.dot_general(
            select,
            keys_values[part],
            (((1,), (0,)), ((), ())),
            preferred_element_type=jnp.float32,
        ).astype(jnp.bfloat16)
        at = 0
        for out in outs:
            out[part] = rows[at : at + out.shape[1]]
            at += out.shape[1]


def edges_kernel(select_ref, peer_ref, *refs):
    select = select_ref[lax.axis_index("th") % 2]
    cut_edges(select, (peer_ref[1], peer_ref[2]), *refs[-2:])


def own_edges_kernel(select_ref, mine_ref, late_ref, near_ref, far_ref, cross_ref):
    half = mine_ref.shape[2]
    select = select_ref[lax.axis_index("th") % 2]
    cut_edges(select, (mine_ref[0], mine_ref[1]), near_ref.at[:, :, :half], far_ref)
    cut_edges(select, (late_ref[1], late_ref[2]), near_ref.at[:, :, half:], cross_ref)


def join_kernel(near_ref, out_ref):
    out_ref[...] = near_ref[:, :, near_ref.shape[2] - out_ref.shape[2] :]


def prepare_kernel(
    valid_ref,
    key_ref,
    query_ref,
    time_ref,
    weight_ref,
    bias_ref,
    gate_ref,
    ok_ref,
    *,
    tile_rows,
    tile_cols,
    edge_rows,
    tiles_down,
):
    row_at = lax.axis_index("th")
    col_at = lax.axis_index("tw")
    key_local, key_col, key_block = (key_ref[i : i + 1] for i in range(3))
    query_row, query_col, query_peer = (query_ref[:, i : i + 1] for i in range(3))
    key_peer = key_block % 2
    row_limit = jnp.zeros_like(key_local)
    col_limit = jnp.zeros_like(key_local)
    shift = jnp.zeros_like(key_local)
    query_limits = []
    toward = 1 - 2 * (row_at % 2)
    for at, step in enumerate((0, toward, -toward)):
        tile_row = row_at + step
        inside = (tile_row >= 0) & (tile_row < tiles_down)
        tile_row = jnp.clip(tile_row, 0, tiles_down - 1)
        for peer in (0, 1):
            side = 1 - col_at if peer else col_at
            rows = jnp.where(inside, valid_ref[side, 0, tile_row], 0)
            cols = valid_ref[side, 1, tile_row]
            block = 2 * at + peer
            row_limit = jnp.where(key_block == block, rows, row_limit)
            col_limit = jnp.where(key_block == block, cols, col_limit)
            if at == 0:
                query_limits.append((rows, cols))
            else:
                shift = jnp.where(key_block == block, step, shift)
    key_local = key_local + jnp.where(shift < 0, tile_rows - edge_rows, 0)
    key_row = key_local + shift * tile_rows
    key_ok = (key_local < row_limit) & (key_col < col_limit)
    key_at = key_col + tile_cols * jnp.where(key_peer > 0, 1 - col_at, col_at)
    query_at = query_col + tile_cols * jnp.where(query_peer > 0, 1 - col_at, col_at)
    row_gap = jnp.abs(query_row - key_row)
    text = key_block == TEXT_BLOCK
    col_gap = jnp.where(key_ok, jnp.abs(query_at - key_at), 2 * HALO + 1)
    for rows in range(HALO):
        for cols in range(HALO):
            near = (row_gap <= rows + 1) & (col_gap <= cols + 1)
            bias_ref[rows * HALO + cols] = jnp.where(near | text, 0.0, NEG)
    row_limit = jnp.where(query_peer > 0, query_limits[1][0], query_limits[0][0])
    col_limit = jnp.where(query_peer > 0, query_limits[1][1], query_limits[0][1])
    query_ok = (query_row < row_limit) & (query_col < col_limit)
    ok_ref[...] = jnp.broadcast_to(jnp.where(query_ok, 1.0, 0.0), ok_ref.shape)
    step = time_ref[...].astype(jnp.float32)
    step = (step / (1.0 + jnp.exp(-step))).astype(jnp.bfloat16)
    gate = jnp.dot(step, weight_ref[...], preferred_element_type=jnp.float32)
    gate = gate.astype(jnp.bfloat16).astype(jnp.float32)
    for pair in range(gate_ref.shape[0]):
        gate_ref[pair] = gate[0:1, pair * LANES : (pair + 1) * LANES]


def attend_kernel(
    extent_ref,
    mine_q_ref,
    mine_kv_ref,
    peer_ref,
    near_mine_ref,
    far_mine_ref,
    text_ref,
    bias_ref,
    gate_ref,
    ok_ref,
    *refs,
    first_pair,
    pairs,
    unroll,
    score_scale,
):
    near_peer_ref, far_peer_ref, own_out_ref, peer_out_ref, key_ref, value_ref = refs
    count = mine_q_ref.shape[1]
    edge = near_mine_ref.shape[1]
    near = 2 * count + 4 * edge
    first_head = lax.axis_index("tw") * (2 * gate_ref.shape[0])
    left = lax.broadcasted_iota(jnp.int32, (1, LANES), 1) < HEAD_DIM
    zero = jnp.zeros((), jnp.bfloat16)

    def lanes_of(turn):
        start = turn * LANES
        if not isinstance(start, int):
            start = pl.multiple_of(start, LANES)
        return pl.ds(start, LANES)

    def score(turn, slot):
        here, whole = lanes_of(turn), lanes_of(first_pair + turn)
        for part, into in ((0, key_ref.at[slot]), (1, value_ref.at[slot])):
            into[0:count] = mine_kv_ref[part, :, whole]
            into[count : 2 * count] = peer_ref[1 + part, :, here]
            at = 2 * count
            for ref, lanes in (
                (near_mine_ref, whole),
                (near_peer_ref, here),
                (far_mine_ref, whole),
                (far_peer_ref, here),
            ):
                into[at : at + edge] = ref[part, :, lanes]
                at += edge
            into[near:] = text_ref[part, :, whole]
        queries = jnp.concatenate([mine_q_ref[0, :, whole], peer_ref[0, :, here]], 0)
        queries = queries * jnp.asarray(score_scale, jnp.bfloat16)
        queries = jnp.concatenate([jnp.where(left, queries, zero), jnp.where(left, zero, queries)], 0)
        return lax.dot_general(
            queries, key_ref[slot], (((1,), (1,)), ((), ())), preferred_element_type=jnp.float32
        )

    def mix(turn, slot, both):
        here = lanes_of(turn)
        weights, shares = [], []
        for side in (0, 1):
            head = first_head + 2 * (first_pair + turn) + side
            reach_rows = jnp.clip(extent_ref[0, head], 1, HALO) - 1
            reach_cols = jnp.clip(extent_ref[1, head], 1, HALO) - 1
            bias = bias_ref[reach_rows * HALO + reach_cols]
            scores = both[2 * count * side : 2 * count * (side + 1)] + bias
            terms = jnp.exp(scores - jnp.max(scores, axis=-1, keepdims=True))
            shares.append(1.0 / jnp.sum(terms, axis=-1, keepdims=True))
            weights.append(terms.astype(jnp.bfloat16))
        sums = lax.dot_general(
            jnp.concatenate(weights, 0),
            value_ref[slot],
            (((1,), (0,)), ((), ())),
            preferred_element_type=jnp.float32,
        )
        attended = jnp.where(left, sums[: 2 * count] * shares[0], sums[2 * count :] * shares[1])
        gated = jnp.where(ok_ref[...] > 0.0, attended * gate_ref[first_pair + turn], 0.0)
        gated = gated.astype(jnp.bfloat16)
        own_out_ref[:, here] = gated[:count]
        peer_out_ref[:, here] = gated[count:]

    def some_pairs(first, size):
        turns = [(first + slot, slot) for slot in range(size)]
        scored = [score(*turn) for turn in turns]
        for turn, both in zip(turns, scored):
            mix(*turn, both)

    steps = -(-pairs // unroll)
    low, extra = divmod(pairs, steps)
    if extra:
        at = 0
        for step in range(steps):
            some_pairs(at, low + (step < extra))
            at += low + (step < extra)
    else:
        lax.fori_loop(0, steps, lambda step, _: some_pairs(step * low, low), None)


def place_kernel(*refs, moves):
    ins, out_ref, sems = refs[:-2], refs[-2], refs[-1]
    col_at = lax.axis_index("tw")
    half = out_ref.shape[1] // 2
    copies = []
    for at, (source, first, other) in enumerate(moves):
        side = 1 - col_at if other else col_at
        ref = ins[source]
        lanes = pl.ds(pl.multiple_of(side * half + first, LANES), ref.shape[1])
        copies.append(pltpu.make_async_copy(ref, out_ref.at[:, lanes], sems.at[at]))
    for copy in copies:
        copy.start()
    for copy in copies:
        copy.wait()


def place(pieces, base, shape, moves):
    vmem = pl.BlockSpec(memory_space=pltpu.VMEM)
    hbm = pl.BlockSpec(memory_space=pltpu.HBM)
    rest = () if base is None else (base,)
    return pl.pallas_call(
        partial(place_kernel, moves=moves),
        out_shape=jax.ShapeDtypeStruct(shape, jnp.bfloat16),
        in_specs=[vmem] * len(pieces) + [hbm] * len(rest),
        out_specs=hbm,
        scratch_shapes=[pltpu.SemaphoreType.DMA((len(moves),))],
        input_output_aliases={} if base is None else {len(pieces): 0},
        compiler_params=pltpu.CompilerParams(vmem_limit_bytes=VMEM_LIMIT),
    )(*pieces, *rest)


def places(frames, tile_rows, tile_cols, edge, text_count, total):
    groups = frames * tile_cols
    blocks = []
    for at, rows in enumerate((tile_rows, HALO, HALO)):
        shape = (frames, tile_cols, rows)
        row = np.broadcast_to(np.arange(rows), shape).reshape(-1)
        col = np.broadcast_to(np.arange(tile_cols)[:, None], shape).reshape(-1)
        for peer in (0, 1):
            blocks.append(np.stack([row, col, 0 * row + 2 * at + peer]))
            if at:
                blocks.append(np.full((3, edge - groups * HALO), TEXT_BLOCK + 1))
    blocks.append(np.full((3, text_count), TEXT_BLOCK))
    query = np.concatenate([blocks[0], blocks[1]], 1)
    used = sum(block.shape[1] for block in blocks)
    blocks.append(np.full((3, total - used), TEXT_BLOCK + 1))
    keys = np.concatenate([np.concatenate(blocks, 1), np.zeros((5, total))]).astype(np.int32)
    query = np.concatenate([query, np.zeros((5, query.shape[1]))]).T.astype(np.int32)
    top = (np.arange(groups)[:, None] * tile_rows + np.arange(HALO)).reshape(-1)
    bottom = top + tile_rows - HALO
    rest = np.full(edge - groups * HALO, -1)
    chosen = np.stack(
        [np.concatenate([bottom, rest, top, rest]), np.concatenate([top, rest, bottom, rest])]
    )
    select = chosen[:, :, None] == np.arange(groups * tile_rows)
    return keys, query, select.astype(jnp.bfloat16)


def swapped_body(queries, video_kv, text_kv, time_embed, gate_weight, window_extent, tile_valid):
    frames, tile_rows, tile_cols, model_width = queries.shape
    half = model_width // 2
    count = frames * tile_rows * tile_cols
    edge = -(-frames * tile_cols * HALO // 8) * 8
    near_keys = 2 * count + 4 * edge
    text_count = text_kv.shape[1]
    total = -(-(near_keys + text_count) // LANES) * LANES
    text_rows = total - near_keys
    tiles_down = lax.axis_size("th")
    swap = [(0, 1), (1, 0)]
    near_pairs = [(i, i ^ 1) for i in range(tiles_down) if i ^ 1 < tiles_down]
    far_pairs = [(i, ((i + 1) ^ 1) - 1) for i in range(1, tiles_down)]
    far_pairs = [(i, j) for i, j in far_pairs if j < tiles_down]
    cross_pairs = [(2 * i + t, 2 * j + 1 - t) for i, j in far_pairs for t in (0, 1)]
    vmem = pl.BlockSpec(memory_space=pltpu.VMEM)
    smem = pl.BlockSpec(memory_space=pltpu.SMEM)
    params = pltpu.CompilerParams(vmem_limit_bytes=VMEM_LIMIT)
    key_places, query_places, select = places(
        frames, tile_rows, tile_cols, edge, text_count, total
    )
    q = jnp.transpose(queries, (0, 2, 1, 3)).reshape(1, count, model_width)
    kv = jnp.transpose(video_kv, (0, 1, 3, 2, 4)).reshape(2, count, model_width)
    q = pltpu.with_memory_space_constraint(q, pltpu.HBM)
    kv = pltpu.with_memory_space_constraint(kv, pltpu.HBM)
    total_pairs = half // LANES
    pieces = []
    first = 0
    for share in CHUNKS:
        pairs = share * total_pairs // sum(CHUNKS)
        pieces.append((first, pairs))
        first += pairs
    head, tail = slice(0, 1), slice(1, 3)
    (first, pairs), (last, rest) = pieces
    low, width, end = first * LANES, pairs * LANES, rest * LANES
    moves = ((0, low, 0, head, True), (1, low, 0, tail, True))
    (early,) = pack(q, kv, [(3, count, width)], moves)
    arrived = [lax.ppermute(early, "tw", swap)]
    shapes = [(3, count, end), (1, count, half), (2, count, half)]
    low = last * LANES
    moves = (
        (0, 0, 1, slice(0, 1), False),
        (1, 0, 2, slice(0, 2), False),
        (0, low, 0, head, True),
        (1, low, 0, tail, True),
    )
    sent, mine_q, mine_kv = pack(q, kv, shapes, moves)
    near, far, crossing = pl.pallas_call(
        own_edges_kernel,
        out_shape=[
            jax.ShapeDtypeStruct((2, edge, half + end), jnp.bfloat16),
            jax.ShapeDtypeStruct((2, edge, half), jnp.bfloat16),
            jax.ShapeDtypeStruct((2, edge, end), jnp.bfloat16),
        ],
        in_specs=[vmem] * 3,
        out_specs=[vmem] * 3,
        compiler_params=params,
        name="own_edges",
    )(select, mine_kv, sent)
    crossed = lax.ppermute(crossing, ("th", "tw"), cross_pairs)
    near_mine = lax.ppermute(near, "th", near_pairs)
    far_mine = lax.ppermute(far, "th", far_pairs)
    arrived.append(lax.ppermute(sent, "tw", swap))
    joined = pl.pallas_call(
        join_kernel,
        out_shape=jax.ShapeDtypeStruct((2, edge, end), jnp.bfloat16),
        in_specs=[vmem],
        out_specs=vmem,
        compiler_params=params,
        name="join",
    )(near_mine)
    joined = lax.ppermute(joined, "tw", swap)
    bias, gate, query_ok = pl.pallas_call(
        partial(
            prepare_kernel,
            tile_rows=tile_rows,
            tile_cols=tile_cols,
            edge_rows=HALO,
            tiles_down=tiles_down,
        ),
        out_shape=[
            jax.ShapeDtypeStruct((HALO * HALO, 2 * count, total), jnp.float32),
            jax.ShapeDtypeStruct((total_pairs, 1, LANES), jnp.float32),
            jax.ShapeDtypeStruct((2 * count, LANES), jnp.float32),
        ],
        in_specs=[smem] + [vmem] * 4,
        out_specs=[vmem] * 3,
        compiler_params=params,
        name="prepare",
    )(
        jnp.transpose(tile_valid.reshape(tiles_down, 2, 2), (1, 2, 0)),
        key_places,
        query_places,
        time_embed.reshape(1, -1),
        gate_weight,
    )
    text = jnp.pad(text_kv, ((0, 0), (0, text_rows - text_count), (0, 0)))
    extents = window_extent.T
    owned, returned = [], []
    for at, ((first, pairs), peer) in enumerate(zip(pieces, arrived)):
        width = pairs * LANES
        near_peer, far_peer = joined, crossed
        if at == 0:
            near, far = pl.pallas_call(
                edges_kernel,
                out_shape=[jax.ShapeDtypeStruct((2, edge, width), jnp.bfloat16)] * 2,
                in_specs=[vmem] * 2 + [pl.BlockSpec(memory_space=pl.ANY)],
                out_specs=[vmem] * 2,
                compiler_params=params,
                name="edges",
            )(select, peer, text)
            far_peer = lax.ppermute(far, "th", far_pairs)
            near_peer = lax.ppermute(near, "th", near_pairs)
        unroll = min(pairs, UNROLL)
        own_out, peer_out = pl.pallas_call(
            partial(
                attend_kernel,
                first_pair=first,
                pairs=pairs,
                unroll=unroll,
                score_scale=HEAD_DIM ** (-0.5),
            ),
            out_shape=[jax.ShapeDtypeStruct((count, width), jnp.bfloat16)] * 2,
            in_specs=[smem] + [vmem] * 11,
            out_specs=[vmem] * 2,
            scratch_shapes=[pltpu.VMEM((unroll, total, LANES), jnp.bfloat16)] * 2,
            compiler_params=params,
        )(
            extents,
            mine_q,
            mine_kv,
            peer,
            near_mine,
            far_mine,
            text,
            bias,
            gate,
            query_ok,
            near_peer,
            far_peer,
        )
        owned.append(own_out)
        returned.append(lax.ppermute(peer_out, "tw", swap))
    starts = [first * LANES for first, _ in pieces]
    early = owned + returned[:-1]
    moves = [(i, low, False) for i, low in enumerate(starts)]
    moves += [(len(owned) + i, low, True) for i, low in enumerate(starts[:-1])]
    result = place(early, None, (count, model_width), tuple(moves))
    moves = ((0, starts[-1], True),)
    result = place(returned[-1:], result, (count, model_width), moves)
    result = result.reshape(frames, tile_cols, tile_rows, model_width)
    return jnp.transpose(result, (0, 2, 1, 3))


def solution(mesh):
    placed = (
        P("vid", "th", "tw", None),
        P(None, "vid", "th", "tw", None),
        P(None, "vid", "tw"),
        P("vid"),
        P(None, "tw"),
        P(),
        P("vid", None, None),
    )
    swapped = mesh.shape["tw"] == 2
    body = swapped_body if swapped else general_body

    return jax.shard_map(
        body, mesh=mesh, in_specs=placed, out_specs=P("vid", "th", "tw", None), check_vma=False
    )
```

```python
import math
from functools import partial

import jax
import jax.numpy as jnp
import numpy as np
from jax import lax
from jax.experimental import pallas as pl
from jax.experimental.pallas import tpu as pltpu
from jax.sharding import PartitionSpec as P


HEAD_DIM = 64
HALO = 3


NEG = -1e30


def extended(cells, sides, width):
    for axis, dim in sides:
        count = lax.axis_size(axis)
        ends = count - 1
        head = lax.slice_in_dim(cells, 0, width, axis=dim)
        tail = lax.slice_in_dim(cells, cells.shape[dim] - width, cells.shape[dim], axis=dim)
        cells = jnp.concatenate(
            [
                lax.ppermute(tail, axis, [(i, (i + 1) % count) for i in range(ends)]),
                cells,
                lax.ppermute(head, axis, [((i + 1) % count, i) for i in range(ends)]),
            ],
            axis=dim,
        )
    return cells


def key_validity(tile_valid, row_at, col_at, tile_rows, tile_cols):
    tiles_down = tile_valid.shape[0]
    tiles_across = tile_valid.shape[1]
    glob_row = row_at * tile_rows + jnp.arange(tile_rows + 2 * HALO, dtype=jnp.int32) - HALO
    glob_col = col_at * tile_cols + jnp.arange(tile_cols + 2 * HALO, dtype=jnp.int32) - HALO
    tile_row = jnp.floor_divide(glob_row, tile_rows)
    tile_col = jnp.floor_divide(glob_col, tile_cols)
    pick_row = (tile_row[:, None] == jnp.arange(tiles_down, dtype=jnp.int32)[None, :]).astype(
        jnp.float32
    )
    pick_col = (tile_col[:, None] == jnp.arange(tiles_across, dtype=jnp.int32)[None, :]).astype(
        jnp.float32
    )
    table = tile_valid.astype(jnp.float32)
    high = lax.Precision.HIGHEST
    limit_rows = jnp.dot(
        jnp.dot(pick_row, table[..., 0], precision=high), pick_col.T, precision=high
    )
    limit_cols = jnp.dot(
        jnp.dot(pick_row, table[..., 1], precision=high), pick_col.T, precision=high
    )
    local_row = (glob_row - tile_row * tile_rows).astype(jnp.float32)
    local_col = (glob_col - tile_col * tile_cols).astype(jnp.float32)
    return (local_row[:, None] < limit_rows) & (local_col[None, :] < limit_cols)


def video_part(
    query_rows,
    video_keys,
    video_values,
    key_ok,
    window_extent,
    frames,
    tile_rows,
    tile_cols,
    score_scale,
):
    count_q, head_count, head_depth = query_rows.shape
    count_k = video_keys.shape[0]
    span_rows = tile_rows + 2 * HALO
    span_cols = tile_cols + 2 * HALO
    per_turn = math.gcd(head_count, 4)
    query_ids = jnp.arange(count_q, dtype=jnp.int32)
    key_ids = jnp.arange(count_k, dtype=jnp.int32)
    query_row = query_ids // tile_cols % tile_rows
    query_col = query_ids % tile_cols
    key_row = key_ids // span_cols % span_rows
    key_col = key_ids % span_cols
    row_gap = jnp.abs(key_row[None, :] - query_row[:, None] - HALO)
    col_gap = jnp.abs(key_col[None, :] - query_col[:, None] - HALO)
    key_flat = jnp.tile(key_ok.reshape(-1), frames)

    def one_group(turn_index, carry):
        video_out, video_max, video_total = carry
        first_head = jnp.asarray(turn_index, jnp.int32) * per_turn
        query_part = lax.dynamic_slice_in_dim(query_rows, first_head, per_turn, 1)
        key_part = lax.dynamic_slice_in_dim(video_keys, first_head, per_turn, 1)
        value_part = lax.dynamic_slice_in_dim(video_values, first_head, per_turn, 1)
        extents = lax.dynamic_slice_in_dim(window_extent, first_head, per_turn, 0)
        allowed = (
            (row_gap[None] <= extents[:, 0][:, None, None])
            & (col_gap[None] <= extents[:, 1][:, None, None])
            & key_flat[None, None, :]
        )
        scores = (
            jnp.einsum("nhd,khd->hnk", query_part, key_part, preferred_element_type=jnp.float32)
            * score_scale
        )
        scores = jnp.where(allowed, scores, NEG)
        maximum = jnp.max(scores, axis=-1)
        exp_terms = jnp.where(allowed, jnp.exp(scores - maximum[..., None]), 0.0)
        totals = jnp.sum(exp_terms, axis=-1)
        weights = exp_terms.astype(jnp.bfloat16)
        partial_value = jnp.einsum(
            "hnk,khd->nhd", weights, value_part, preferred_element_type=jnp.float32
        )
        video_out = lax.dynamic_update_slice_in_dim(video_out, partial_value, first_head, 1)
        video_max = lax.dynamic_update_slice_in_dim(video_max, maximum, first_head, 0)
        video_total = lax.dynamic_update_slice_in_dim(video_total, totals, first_head, 0)
        return (video_out, video_max, video_total)

    initial = (
        jnp.zeros((count_q, head_count, head_depth), jnp.float32),
        jnp.zeros((head_count, count_q), jnp.float32),
        jnp.zeros((head_count, count_q), jnp.float32),
    )
    return lax.fori_loop(0, head_count // per_turn, one_group, initial)


def text_part(query_rows, text_keys, text_values, score_scale):
    scores = (
        jnp.einsum("nhd,thd->nht", query_rows, text_keys, preferred_element_type=jnp.float32)
        * score_scale
    )
    maximum = jnp.max(scores, axis=-1)
    exp_terms = jnp.exp(scores - maximum[..., None])
    totals = jnp.sum(exp_terms, axis=-1)
    partial_value = jnp.einsum(
        "nht,thd->nhd",
        exp_terms.astype(jnp.bfloat16),
        text_values,
        preferred_element_type=jnp.float32,
    )
    return (partial_value, maximum, totals)


def combine(video_out, video_max, video_total, text_out, text_max, text_total):
    max_v = video_max.T
    total_v = video_total.T
    joint_max = jnp.maximum(max_v, text_max)
    scale_v = jnp.exp(max_v - joint_max)
    scale_t = jnp.exp(text_max - joint_max)
    denom = total_v * scale_v + text_total * scale_t
    return (video_out * scale_v[..., None] + text_out * scale_t[..., None]) / denom[..., None]


def attend_tile(
    query_block,
    kv_block,
    text_keys,
    text_values,
    extents,
    gate_vec,
    key_ok,
    tile_rows,
    tile_cols,
    score_scale,
):
    frames = query_block.shape[0]
    width = query_block.shape[3]
    head_count = width // HEAD_DIM
    query_rows = query_block.reshape(-1, head_count, HEAD_DIM)
    video_keys = kv_block[0].reshape(-1, head_count, HEAD_DIM)
    video_values = kv_block[1].reshape(-1, head_count, HEAD_DIM)
    video_out, video_max, video_total = video_part(
        query_rows,
        video_keys,
        video_values,
        key_ok,
        extents,
        frames,
        tile_rows,
        tile_cols,
        score_scale,
    )
    text_out, text_max, text_total = text_part(query_rows, text_keys, text_values, score_scale)
    attended = combine(video_out, video_max, video_total, text_out, text_max, text_total)
    attended = attended.reshape(frames, tile_rows, tile_cols, width)
    query_ok = key_ok[HALO : HALO + tile_rows, HALO : HALO + tile_cols]
    result = jnp.where(query_ok[None, :, :, None], gate_vec.astype(jnp.float32) * attended, 0.0)
    return result.astype(jnp.bfloat16)


def general_body(queries, video_kv, text_kv, time_embed, gate_weight, window_extent, tile_valid):
    _, tile_rows, tile_cols, model_width = queries.shape
    head_count = model_width // HEAD_DIM
    score_scale = HEAD_DIM ** (-0.5)
    text_count = text_kv.shape[1]
    row_at = lax.axis_index("th")
    col_at = lax.axis_index("tw")
    mod_in = jax.nn.silu(time_embed.astype(jnp.float32)).astype(jnp.bfloat16)
    gate_part = jnp.dot(mod_in[None, :], gate_weight, preferred_element_type=jnp.float32)[0].astype(
        jnp.bfloat16
    )
    padded = extended(video_kv, (("th", 2), ("tw", 3)), HALO)
    text_full, gate_full = (
        lax.all_gather(text_kv, "tw", axis=2, tiled=True),
        lax.all_gather(gate_part, "tw", axis=0, tiled=True),
    )
    text_keys = text_full[0].reshape(text_count, head_count, HEAD_DIM)
    text_values = text_full[1].reshape(text_count, head_count, HEAD_DIM)
    key_ok = key_validity(tile_valid, row_at, col_at, tile_rows, tile_cols)
    return attend_tile(
        queries,
        padded,
        text_keys,
        text_values,
        window_extent,
        gate_full,
        key_ok,
        tile_rows,
        tile_cols,
        score_scale,
    )


LANES = 128
CHUNKS = (7, 5)
UNROLL = 4
TEXT_BLOCK = 6
VMEM_LIMIT = 16 * 2**20


def pack_kernel(q_ref, kv_ref, *refs, moves):
    outs, sems = refs[:-1], refs[-1]
    col_at = lax.axis_index("tw")
    half = q_ref.shape[2] // 2
    copies = []
    for source, first, out, slot, other in moves:
        to = outs[out].at[slot]
        side = 1 - col_at if other else col_at
        lanes = pl.ds(pl.multiple_of(side * half + first, LANES), to.shape[2])
        ref = q_ref if source == 0 else kv_ref
        copies.append(pltpu.make_async_copy(ref.at[:, :, lanes], to, sems.at[len(copies)]))
    for copy in copies:
        copy.start()
    for copy in copies:
        copy.wait()


def pack(q, kv, shapes, moves):
    return pl.pallas_call(
        partial(pack_kernel, moves=moves),
        out_shape=[jax.ShapeDtypeStruct(shape, q.dtype) for shape in shapes],
        in_specs=[pl.BlockSpec(memory_space=pltpu.HBM)] * 2,
        out_specs=[pl.BlockSpec(memory_space=pltpu.VMEM)] * len(shapes),
        scratch_shapes=[pltpu.SemaphoreType.DMA((len(moves),))],
        compiler_params=pltpu.CompilerParams(vmem_limit_bytes=VMEM_LIMIT),
    )(q, kv)


def cut_edges(select, keys_values, *outs):
    for part in (0, 1):
        rows = lax.dot_general(
            select,
            keys_values[part],
            (((1,), (0,)), ((), ())),
            preferred_element_type=jnp.float32,
        ).astype(jnp.bfloat16)
        at = 0
        for out in outs:
            out[part] = rows[at : at + out.shape[1]]
            at += out.shape[1]


def edges_kernel(select_ref, peer_ref, *refs):
    near_ref = refs[-1]
    select = select_ref[lax.axis_index("th") % 2, : near_ref.shape[1]]
    cut_edges(select, (peer_ref[1], peer_ref[2]), near_ref)


def own_edges_kernel(
    select_ref, mine_ref, early_ref, late_ref, near_ref, far_ref, first_ref, second_ref
):
    half = mine_ref.shape[2]
    select = select_ref[lax.axis_index("th") % 2]
    cut_edges(select[far_ref.shape[1] :], (early_ref[1], early_ref[2]), first_ref)
    cut_edges(select, (mine_ref[0], mine_ref[1]), near_ref.at[:, :, :half], far_ref)
    cut_edges(select, (late_ref[1], late_ref[2]), near_ref.at[:, :, half:], second_ref)


def join_kernel(near_ref, out_ref):
    out_ref[...] = near_ref[:, :, near_ref.shape[2] - out_ref.shape[2] :]


def prepare_kernel(
    valid_ref,
    key_ref,
    query_ref,
    time_ref,
    weight_ref,
    bias_ref,
    gate_ref,
    ok_ref,
    *,
    tile_rows,
    tile_cols,
    edge_rows,
    tiles_down,
):
    row_at = lax.axis_index("th")
    col_at = lax.axis_index("tw")
    key_local, key_col, key_block = (key_ref[i : i + 1] for i in range(3))
    query_row, query_col, query_peer = (query_ref[:, i : i + 1] for i in range(3))
    key_peer = key_block % 2
    row_limit = jnp.zeros_like(key_local)
    col_limit = jnp.zeros_like(key_local)
    shift = jnp.zeros_like(key_local)
    query_limits = []
    toward = 1 - 2 * (row_at % 2)
    for at, step in enumerate((0, toward, -toward)):
        tile_row = row_at + step
        inside = (tile_row >= 0) & (tile_row < tiles_down)
        tile_row = jnp.clip(tile_row, 0, tiles_down - 1)
        for peer in (0, 1):
            side = 1 - col_at if peer else col_at
            rows = jnp.where(inside, valid_ref[side, 0, tile_row], 0)
            cols = valid_ref[side, 1, tile_row]
            block = 2 * at + peer
            row_limit = jnp.where(key_block == block, rows, row_limit)
            col_limit = jnp.where(key_block == block, cols, col_limit)
            if at == 0:
                query_limits.append((rows, cols))
            else:
                shift = jnp.where(key_block == block, step, shift)
    key_local = key_local + jnp.where(shift < 0, tile_rows - edge_rows, 0)
    key_row = key_local + shift * tile_rows
    key_ok = (key_local < row_limit) & (key_col < col_limit)
    key_at = key_col + tile_cols * jnp.where(key_peer > 0, 1 - col_at, col_at)
    query_at = query_col + tile_cols * jnp.where(query_peer > 0, 1 - col_at, col_at)
    row_gap = jnp.abs(query_row - key_row)
    text = key_block == TEXT_BLOCK
    col_gap = jnp.where(key_ok, jnp.abs(query_at - key_at), 2 * HALO + 1)
    for rows in range(HALO):
        for cols in range(HALO):
            near = (row_gap <= rows + 1) & (col_gap <= cols + 1)
            bias_ref[rows * HALO + cols] = jnp.where(near | text, 0.0, NEG)
    row_limit = jnp.where(query_peer > 0, query_limits[1][0], query_limits[0][0])
    col_limit = jnp.where(query_peer > 0, query_limits[1][1], query_limits[0][1])
    query_ok = (query_row < row_limit) & (query_col < col_limit)
    ok_ref[...] = jnp.broadcast_to(jnp.where(query_ok, 1.0, 0.0), ok_ref.shape)
    step = time_ref[...].astype(jnp.float32)
    step = (step / (1.0 + jnp.exp(-step))).astype(jnp.bfloat16)
    gate = jnp.dot(step, weight_ref[...], preferred_element_type=jnp.float32)
    gate = gate.astype(jnp.bfloat16).astype(jnp.float32)
    for pair in range(gate_ref.shape[0]):
        gate_ref[pair] = gate[0:1, pair * LANES : (pair + 1) * LANES]


def attend_kernel(
    extent_ref,
    mine_q_ref,
    mine_kv_ref,
    peer_ref,
    near_mine_ref,
    far_mine_ref,
    text_ref,
    bias_ref,
    gate_ref,
    ok_ref,
    *refs,
    first_pair,
    pairs,
    unroll,
    score_scale,
):
    near_peer_ref, far_peer_ref, own_out_ref, peer_out_ref, key_ref, value_ref = refs
    count = mine_q_ref.shape[1]
    edge = near_mine_ref.shape[1]
    near = 2 * count + 4 * edge
    first_head = lax.axis_index("tw") * (2 * gate_ref.shape[0])
    left = lax.broadcasted_iota(jnp.int32, (1, LANES), 1) < HEAD_DIM
    zero = jnp.zeros((), jnp.bfloat16)

    def lanes_of(turn):
        start = turn * LANES
        if not isinstance(start, int):
            start = pl.multiple_of(start, LANES)
        return pl.ds(start, LANES)

    def score(turn, slot):
        here, whole = lanes_of(turn), lanes_of(first_pair + turn)
        for part, into in ((0, key_ref.at[slot]), (1, value_ref.at[slot])):
            into[0:count] = mine_kv_ref[part, :, whole]
            into[count : 2 * count] = peer_ref[1 + part, :, here]
            at = 2 * count
            for ref, lanes in (
                (near_mine_ref, whole),
                (near_peer_ref, here),
                (far_mine_ref, whole),
                (far_peer_ref, here),
            ):
                into[at : at + edge] = ref[part, :, lanes]
                at += edge
            into[near:] = text_ref[part, :, whole]
        queries = jnp.concatenate([mine_q_ref[0, :, whole], peer_ref[0, :, here]], 0)
        queries = queries * jnp.asarray(score_scale, jnp.bfloat16)
        queries = jnp.concatenate([jnp.where(left, queries, zero), jnp.where(left, zero, queries)], 0)
        return lax.dot_general(
            queries, key_ref[slot], (((1,), (1,)), ((), ())), preferred_element_type=jnp.float32
        )

    def mix(turn, slot, both):
        here = lanes_of(turn)
        weights, shares = [], []
        for side in (0, 1):
            head = first_head + 2 * (first_pair + turn) + side
            reach_rows = jnp.clip(extent_ref[0, head], 1, HALO) - 1
            reach_cols = jnp.clip(extent_ref[1, head], 1, HALO) - 1
            bias = bias_ref[reach_rows * HALO + reach_cols]
            scores = both[2 * count * side : 2 * count * (side + 1)] + bias
            terms = jnp.exp(scores - jnp.max(scores, axis=-1, keepdims=True))
            shares.append(1.0 / jnp.sum(terms, axis=-1, keepdims=True))
            weights.append(terms.astype(jnp.bfloat16))
        sums = lax.dot_general(
            jnp.concatenate(weights, 0),
            value_ref[slot],
            (((1,), (0,)), ((), ())),
            preferred_element_type=jnp.float32,
        )
        attended = jnp.where(left, sums[: 2 * count] * shares[0], sums[2 * count :] * shares[1])
        gated = jnp.where(ok_ref[...] > 0.0, attended * gate_ref[first_pair + turn], 0.0)
        gated = gated.astype(jnp.bfloat16)
        own_out_ref[:, here] = gated[:count]
        peer_out_ref[:, here] = gated[count:]

    def some_pairs(first, size):
        turns = [(first + slot, slot) for slot in range(size)]
        scored = [score(*turn) for turn in turns]
        for turn, both in zip(turns, scored):
            mix(*turn, both)

    steps = -(-pairs // unroll)
    low, extra = divmod(pairs, steps)
    if extra:
        at = 0
        for step in range(steps):
            some_pairs(at, low + (step < extra))
            at += low + (step < extra)
    else:
        lax.fori_loop(0, steps, lambda step, _: some_pairs(step * low, low), None)


def place_kernel(*refs, moves):
    ins, out_ref, sems = refs[:-2], refs[-2], refs[-1]
    col_at = lax.axis_index("tw")
    half = out_ref.shape[1] // 2
    copies = []
    for at, (source, first, other) in enumerate(moves):
        side = 1 - col_at if other else col_at
        ref = ins[source]
        lanes = pl.ds(pl.multiple_of(side * half + first, LANES), ref.shape[1])
        copies.append(pltpu.make_async_copy(ref, out_ref.at[:, lanes], sems.at[at]))
    for copy in copies:
        copy.start()
    for copy in copies:
        copy.wait()


def place(pieces, base, shape, moves):
    vmem = pl.BlockSpec(memory_space=pltpu.VMEM)
    hbm = pl.BlockSpec(memory_space=pltpu.HBM)
    rest = () if base is None else (base,)
    return pl.pallas_call(
        partial(place_kernel, moves=moves),
        out_shape=jax.ShapeDtypeStruct(shape, jnp.bfloat16),
        in_specs=[vmem] * len(pieces) + [hbm] * len(rest),
        out_specs=hbm,
        scratch_shapes=[pltpu.SemaphoreType.DMA((len(moves),))],
        input_output_aliases={} if base is None else {len(pieces): 0},
        compiler_params=pltpu.CompilerParams(vmem_limit_bytes=VMEM_LIMIT),
    )(*pieces, *rest)


def places(frames, tile_rows, tile_cols, edge, text_count, total):
    groups = frames * tile_cols
    blocks = []
    for at, rows in enumerate((tile_rows, HALO, HALO)):
        shape = (frames, tile_cols, rows)
        row = np.broadcast_to(np.arange(rows), shape).reshape(-1)
        col = np.broadcast_to(np.arange(tile_cols)[:, None], shape).reshape(-1)
        for peer in (0, 1):
            blocks.append(np.stack([row, col, 0 * row + 2 * at + peer]))
            if at:
                blocks.append(np.full((3, edge - groups * HALO), TEXT_BLOCK + 1))
    blocks.append(np.full((3, text_count), TEXT_BLOCK))
    query = np.concatenate([blocks[0], blocks[1]], 1)
    used = sum(block.shape[1] for block in blocks)
    blocks.append(np.full((3, total - used), TEXT_BLOCK + 1))
    keys = np.concatenate([np.concatenate(blocks, 1), np.zeros((5, total))]).astype(np.int32)
    query = np.concatenate([query, np.zeros((5, query.shape[1]))]).T.astype(np.int32)
    top = (np.arange(groups)[:, None] * tile_rows + np.arange(HALO)).reshape(-1)
    bottom = top + tile_rows - HALO
    rest = np.full(edge - groups * HALO, -1)
    chosen = np.stack(
        [np.concatenate([bottom, rest, top, rest]), np.concatenate([top, rest, bottom, rest])]
    )
    select = chosen[:, :, None] == np.arange(groups * tile_rows)
    return keys, query, select.astype(jnp.bfloat16)


def swapped_body(queries, video_kv, text_kv, time_embed, gate_weight, window_extent, tile_valid):
    frames, tile_rows, tile_cols, model_width = queries.shape
    half = model_width // 2
    count = frames * tile_rows * tile_cols
    edge = -(-frames * tile_cols * HALO // 8) * 8
    near_keys = 2 * count + 4 * edge
    text_count = text_kv.shape[1]
    total = -(-(near_keys + text_count) // LANES) * LANES
    text_rows = total - near_keys
    tiles_down = lax.axis_size("th")
    swap = [(0, 1), (1, 0)]
    near_pairs = [(i, i ^ 1) for i in range(tiles_down) if i ^ 1 < tiles_down]
    far_pairs = [(i, ((i + 1) ^ 1) - 1) for i in range(1, tiles_down)]
    far_pairs = [(i, j) for i, j in far_pairs if j < tiles_down]
    cross_pairs = [(2 * i + t, 2 * j + 1 - t) for i, j in far_pairs for t in (0, 1)]
    vmem = pl.BlockSpec(memory_space=pltpu.VMEM)
    smem = pl.BlockSpec(memory_space=pltpu.SMEM)
    params = pltpu.CompilerParams(vmem_limit_bytes=VMEM_LIMIT)
    key_places, query_places, select = places(
        frames, tile_rows, tile_cols, edge, text_count, total
    )
    q = jnp.transpose(queries, (0, 2, 1, 3)).reshape(1, count, model_width)
    kv = jnp.transpose(video_kv, (0, 1, 3, 2, 4)).reshape(2, count, model_width)
    q = pltpu.with_memory_space_constraint(q, pltpu.HBM)
    kv = pltpu.with_memory_space_constraint(kv, pltpu.HBM)
    total_pairs = half // LANES
    pieces = []
    first = 0
    for share in CHUNKS:
        pairs = share * total_pairs // sum(CHUNKS)
        pieces.append((first, pairs))
        first += pairs
    head, tail = slice(0, 1), slice(1, 3)
    (first, pairs), (last, rest) = pieces
    low, width, end = first * LANES, pairs * LANES, rest * LANES
    moves = ((0, low, 0, head, True), (1, low, 0, tail, True))
    (early,) = pack(q, kv, [(3, count, width)], moves)
    arrived = [lax.ppermute(early, "tw", swap)]
    shapes = [(3, count, end), (1, count, half), (2, count, half)]
    low = last * LANES
    moves = (
        (0, 0, 1, slice(0, 1), False),
        (1, 0, 2, slice(0, 2), False),
        (0, low, 0, head, True),
        (1, low, 0, tail, True),
    )
    sent, mine_q, mine_kv = pack(q, kv, shapes, moves)
    near, far, *crossing = pl.pallas_call(
        own_edges_kernel,
        out_shape=[
            jax.ShapeDtypeStruct((2, edge, half + end), jnp.bfloat16),
            jax.ShapeDtypeStruct((2, edge, half), jnp.bfloat16),
            jax.ShapeDtypeStruct((2, edge, width), jnp.bfloat16),
            jax.ShapeDtypeStruct((2, edge, end), jnp.bfloat16),
        ],
        in_specs=[vmem] * 4,
        out_specs=[vmem] * 4,
        compiler_params=params,
        name="own_edges",
    )(select, mine_kv, early, sent)
    crossed = []
    for rows in crossing:
        crossed.append(lax.ppermute(rows, ("th", "tw"), cross_pairs))
    near_mine = lax.ppermute(near, "th", near_pairs)
    far_mine = lax.ppermute(far, "th", far_pairs)
    arrived.append(lax.ppermute(sent, "tw", swap))
    joined = pl.pallas_call(
        join_kernel,
        out_shape=jax.ShapeDtypeStruct((2, edge, end), jnp.bfloat16),
        in_specs=[vmem],
        out_specs=vmem,
        compiler_params=params,
        name="join",
    )(near_mine)
    joined = lax.ppermute(joined, "tw", swap)
    bias, gate, query_ok = pl.pallas_call(
        partial(
            prepare_kernel,
            tile_rows=tile_rows,
            tile_cols=tile_cols,
            edge_rows=HALO,
            tiles_down=tiles_down,
        ),
        out_shape=[
            jax.ShapeDtypeStruct((HALO * HALO, 2 * count, total), jnp.float32),
            jax.ShapeDtypeStruct((total_pairs, 1, LANES), jnp.float32),
            jax.ShapeDtypeStruct((2 * count, LANES), jnp.float32),
        ],
        in_specs=[smem] + [vmem] * 4,
        out_specs=[vmem] * 3,
        compiler_params=params,
        name="prepare",
    )(
        jnp.transpose(tile_valid.reshape(tiles_down, 2, 2), (1, 2, 0)),
        key_places,
        query_places,
        time_embed.reshape(1, -1),
        gate_weight,
    )
    text = jnp.pad(text_kv, ((0, 0), (0, text_rows - text_count), (0, 0)))
    extents = window_extent.T
    owned, returned = [], []
    for at, ((first, pairs), peer) in enumerate(zip(pieces, arrived)):
        width = pairs * LANES
        near_peer, far_peer = joined, crossed[at]
        if at == 0:
            near = pl.pallas_call(
                edges_kernel,
                out_shape=jax.ShapeDtypeStruct((2, edge, width), jnp.bfloat16),
                in_specs=[vmem] * 2 + [pl.BlockSpec(memory_space=pl.ANY)],
                out_specs=vmem,
                compiler_params=params,
                name="edges",
            )(select, peer, text)
            near_peer = lax.ppermute(near, "th", near_pairs)
        unroll = min(pairs, UNROLL)
        own_out, peer_out = pl.pallas_call(
            partial(
                attend_kernel,
                first_pair=first,
                pairs=pairs,
                unroll=unroll,
                score_scale=HEAD_DIM ** (-0.5),
            ),
            out_shape=[jax.ShapeDtypeStruct((count, width), jnp.bfloat16)] * 2,
            in_specs=[smem] + [vmem] * 11,
            out_specs=[vmem] * 2,
            scratch_shapes=[pltpu.VMEM((unroll, total, LANES), jnp.bfloat16)] * 2,
            compiler_params=params,
        )(
            extents,
            mine_q,
            mine_kv,
            peer,
            near_mine,
            far_mine,
            text,
            bias,
            gate,
            query_ok,
            near_peer,
            far_peer,
        )
        owned.append(own_out)
        returned.append(lax.ppermute(peer_out, "tw", swap))
    starts = [first * LANES for first, _ in pieces]
    early = owned + returned[:-1]
    moves = [(i, low, False) for i, low in enumerate(starts)]
    moves += [(len(owned) + i, low, True) for i, low in enumerate(starts[:-1])]
    result = place(early, None, (count, model_width), tuple(moves))
    moves = ((0, starts[-1], True),)
    result = place(returned[-1:], result, (count, model_width), moves)
    result = result.reshape(frames, tile_cols, tile_rows, model_width)
    return jnp.transpose(result, (0, 2, 1, 3))


def solution(mesh):
    placed = (
        P("vid", "th", "tw", None),
        P(None, "vid", "th", "tw", None),
        P(None, "vid", "tw"),
        P("vid"),
        P(None, "tw"),
        P(),
        P("vid", None, None),
    )
    swapped = mesh.shape["tw"] == 2
    body = swapped_body if swapped else general_body

    return jax.shard_map(
        body, mesh=mesh, in_specs=placed, out_specs=P("vid", "th", "tw", None), check_vma=False
    )
```

```python
import math
from functools import partial

import jax
import jax.numpy as jnp
import numpy as np
from jax import lax
from jax.experimental import pallas as pl
from jax.experimental.pallas import tpu as pltpu
from jax.sharding import PartitionSpec as P


HEAD_DIM = 64
HALO = 3


NEG = -1e30


def extended(cells, sides, width):
    for axis, dim in sides:
        count = lax.axis_size(axis)
        ends = count - 1
        head = lax.slice_in_dim(cells, 0, width, axis=dim)
        tail = lax.slice_in_dim(cells, cells.shape[dim] - width, cells.shape[dim], axis=dim)
        cells = jnp.concatenate(
            [
                lax.ppermute(tail, axis, [(i, (i + 1) % count) for i in range(ends)]),
                cells,
                lax.ppermute(head, axis, [((i + 1) % count, i) for i in range(ends)]),
            ],
            axis=dim,
        )
    return cells


def key_validity(tile_valid, row_at, col_at, tile_rows, tile_cols):
    tiles_down = tile_valid.shape[0]
    tiles_across = tile_valid.shape[1]
    glob_row = row_at * tile_rows + jnp.arange(tile_rows + 2 * HALO, dtype=jnp.int32) - HALO
    glob_col = col_at * tile_cols + jnp.arange(tile_cols + 2 * HALO, dtype=jnp.int32) - HALO
    tile_row = jnp.floor_divide(glob_row, tile_rows)
    tile_col = jnp.floor_divide(glob_col, tile_cols)
    pick_row = (tile_row[:, None] == jnp.arange(tiles_down, dtype=jnp.int32)[None, :]).astype(
        jnp.float32
    )
    pick_col = (tile_col[:, None] == jnp.arange(tiles_across, dtype=jnp.int32)[None, :]).astype(
        jnp.float32
    )
    table = tile_valid.astype(jnp.float32)
    high = lax.Precision.HIGHEST
    limit_rows = jnp.dot(
        jnp.dot(pick_row, table[..., 0], precision=high), pick_col.T, precision=high
    )
    limit_cols = jnp.dot(
        jnp.dot(pick_row, table[..., 1], precision=high), pick_col.T, precision=high
    )
    local_row = (glob_row - tile_row * tile_rows).astype(jnp.float32)
    local_col = (glob_col - tile_col * tile_cols).astype(jnp.float32)
    return (local_row[:, None] < limit_rows) & (local_col[None, :] < limit_cols)


def video_part(
    query_rows,
    video_keys,
    video_values,
    key_ok,
    window_extent,
    frames,
    tile_rows,
    tile_cols,
    score_scale,
):
    count_q, head_count, head_depth = query_rows.shape
    count_k = video_keys.shape[0]
    span_rows = tile_rows + 2 * HALO
    span_cols = tile_cols + 2 * HALO
    per_turn = math.gcd(head_count, 4)
    query_ids = jnp.arange(count_q, dtype=jnp.int32)
    key_ids = jnp.arange(count_k, dtype=jnp.int32)
    query_row = query_ids // tile_cols % tile_rows
    query_col = query_ids % tile_cols
    key_row = key_ids // span_cols % span_rows
    key_col = key_ids % span_cols
    row_gap = jnp.abs(key_row[None, :] - query_row[:, None] - HALO)
    col_gap = jnp.abs(key_col[None, :] - query_col[:, None] - HALO)
    key_flat = jnp.tile(key_ok.reshape(-1), frames)

    def one_group(turn_index, carry):
        video_out, video_max, video_total = carry
        first_head = jnp.asarray(turn_index, jnp.int32) * per_turn
        query_part = lax.dynamic_slice_in_dim(query_rows, first_head, per_turn, 1)
        key_part = lax.dynamic_slice_in_dim(video_keys, first_head, per_turn, 1)
        value_part = lax.dynamic_slice_in_dim(video_values, first_head, per_turn, 1)
        extents = lax.dynamic_slice_in_dim(window_extent, first_head, per_turn, 0)
        allowed = (
            (row_gap[None] <= extents[:, 0][:, None, None])
            & (col_gap[None] <= extents[:, 1][:, None, None])
            & key_flat[None, None, :]
        )
        scores = (
            jnp.einsum("nhd,khd->hnk", query_part, key_part, preferred_element_type=jnp.float32)
            * score_scale
        )
        scores = jnp.where(allowed, scores, NEG)
        maximum = jnp.max(scores, axis=-1)
        exp_terms = jnp.where(allowed, jnp.exp(scores - maximum[..., None]), 0.0)
        totals = jnp.sum(exp_terms, axis=-1)
        weights = exp_terms.astype(jnp.bfloat16)
        partial_value = jnp.einsum(
            "hnk,khd->nhd", weights, value_part, preferred_element_type=jnp.float32
        )
        video_out = lax.dynamic_update_slice_in_dim(video_out, partial_value, first_head, 1)
        video_max = lax.dynamic_update_slice_in_dim(video_max, maximum, first_head, 0)
        video_total = lax.dynamic_update_slice_in_dim(video_total, totals, first_head, 0)
        return (video_out, video_max, video_total)

    initial = (
        jnp.zeros((count_q, head_count, head_depth), jnp.float32),
        jnp.zeros((head_count, count_q), jnp.float32),
        jnp.zeros((head_count, count_q), jnp.float32),
    )
    return lax.fori_loop(0, head_count // per_turn, one_group, initial)


def text_part(query_rows, text_keys, text_values, score_scale):
    scores = (
        jnp.einsum("nhd,thd->nht", query_rows, text_keys, preferred_element_type=jnp.float32)
        * score_scale
    )
    maximum = jnp.max(scores, axis=-1)
    exp_terms = jnp.exp(scores - maximum[..., None])
    totals = jnp.sum(exp_terms, axis=-1)
    partial_value = jnp.einsum(
        "nht,thd->nhd",
        exp_terms.astype(jnp.bfloat16),
        text_values,
        preferred_element_type=jnp.float32,
    )
    return (partial_value, maximum, totals)


def combine(video_out, video_max, video_total, text_out, text_max, text_total):
    max_v = video_max.T
    total_v = video_total.T
    joint_max = jnp.maximum(max_v, text_max)
    scale_v = jnp.exp(max_v - joint_max)
    scale_t = jnp.exp(text_max - joint_max)
    denom = total_v * scale_v + text_total * scale_t
    return (video_out * scale_v[..., None] + text_out * scale_t[..., None]) / denom[..., None]


def attend_tile(
    query_block,
    kv_block,
    text_keys,
    text_values,
    extents,
    gate_vec,
    key_ok,
    tile_rows,
    tile_cols,
    score_scale,
):
    frames = query_block.shape[0]
    width = query_block.shape[3]
    head_count = width // HEAD_DIM
    query_rows = query_block.reshape(-1, head_count, HEAD_DIM)
    video_keys = kv_block[0].reshape(-1, head_count, HEAD_DIM)
    video_values = kv_block[1].reshape(-1, head_count, HEAD_DIM)
    video_out, video_max, video_total = video_part(
        query_rows,
        video_keys,
        video_values,
        key_ok,
        extents,
        frames,
        tile_rows,
        tile_cols,
        score_scale,
    )
    text_out, text_max, text_total = text_part(query_rows, text_keys, text_values, score_scale)
    attended = combine(video_out, video_max, video_total, text_out, text_max, text_total)
    attended = attended.reshape(frames, tile_rows, tile_cols, width)
    query_ok = key_ok[HALO : HALO + tile_rows, HALO : HALO + tile_cols]
    result = jnp.where(query_ok[None, :, :, None], gate_vec.astype(jnp.float32) * attended, 0.0)
    return result.astype(jnp.bfloat16)


def general_body(queries, video_kv, text_kv, time_embed, gate_weight, window_extent, tile_valid):
    _, tile_rows, tile_cols, model_width = queries.shape
    head_count = model_width // HEAD_DIM
    score_scale = HEAD_DIM ** (-0.5)
    text_count = text_kv.shape[1]
    row_at = lax.axis_index("th")
    col_at = lax.axis_index("tw")
    mod_in = jax.nn.silu(time_embed.astype(jnp.float32)).astype(jnp.bfloat16)
    gate_part = jnp.dot(mod_in[None, :], gate_weight, preferred_element_type=jnp.float32)[0].astype(
        jnp.bfloat16
    )
    padded = extended(video_kv, (("th", 2), ("tw", 3)), HALO)
    text_full, gate_full = (
        lax.all_gather(text_kv, "tw", axis=2, tiled=True),
        lax.all_gather(gate_part, "tw", axis=0, tiled=True),
    )
    text_keys = text_full[0].reshape(text_count, head_count, HEAD_DIM)
    text_values = text_full[1].reshape(text_count, head_count, HEAD_DIM)
    key_ok = key_validity(tile_valid, row_at, col_at, tile_rows, tile_cols)
    return attend_tile(
        queries,
        padded,
        text_keys,
        text_values,
        window_extent,
        gate_full,
        key_ok,
        tile_rows,
        tile_cols,
        score_scale,
    )


LANES = 128
CHUNKS = (7, 5)
UNROLL = 4
TEXT_BLOCK = 6
VMEM_LIMIT = 16 * 2**20


def pack_kernel(q_ref, kv_ref, *refs, moves):
    outs, sems = refs[:-1], refs[-1]
    col_at = lax.axis_index("tw")
    half = q_ref.shape[2] // 2
    copies = []
    for source, first, out, slot, other in moves:
        to = outs[out].at[slot]
        side = 1 - col_at if other else col_at
        lanes = pl.ds(pl.multiple_of(side * half + first, LANES), to.shape[2])
        ref = q_ref if source == 0 else kv_ref
        copies.append(pltpu.make_async_copy(ref.at[:, :, lanes], to, sems.at[len(copies)]))
    for copy in copies:
        copy.start()
    for copy in copies:
        copy.wait()


def pack(q, kv, shapes, moves):
    return pl.pallas_call(
        partial(pack_kernel, moves=moves),
        out_shape=[jax.ShapeDtypeStruct(shape, q.dtype) for shape in shapes],
        in_specs=[pl.BlockSpec(memory_space=pltpu.HBM)] * 2,
        out_specs=[pl.BlockSpec(memory_space=pltpu.VMEM)] * len(shapes),
        scratch_shapes=[pltpu.SemaphoreType.DMA((len(moves),))],
        compiler_params=pltpu.CompilerParams(vmem_limit_bytes=VMEM_LIMIT),
    )(q, kv)


def cut_edges(select, keys_values, *outs):
    for part in (0, 1):
        rows = lax.dot_general(
            select,
            keys_values[part],
            (((1,), (0,)), ((), ())),
            preferred_element_type=jnp.float32,
        ).astype(jnp.bfloat16)
        at = 0
        for out in outs:
            out[part] = rows[at : at + out.shape[1]]
            at += out.shape[1]


def edges_kernel(select_ref, peer_ref, *refs):
    near_ref = refs[-1]
    select = select_ref[lax.axis_index("th") % 2, : near_ref.shape[1]]
    cut_edges(select, (peer_ref[1], peer_ref[2]), near_ref)


def own_edges_kernel(
    select_ref, mine_ref, early_ref, late_ref, near_ref, far_ref, first_ref, second_ref
):
    select = select_ref[lax.axis_index("th") % 2]
    cut_edges(select[far_ref.shape[1] :], (early_ref[1], early_ref[2]), first_ref)
    cut_edges(select, (mine_ref[0], mine_ref[1]), near_ref, far_ref)
    cut_edges(select[far_ref.shape[1] :], (late_ref[1], late_ref[2]), second_ref)


def prepare_kernel(
    valid_ref,
    key_ref,
    query_ref,
    time_ref,
    weight_ref,
    bias_ref,
    gate_ref,
    ok_ref,
    *,
    tile_rows,
    tile_cols,
    edge_rows,
    tiles_down,
):
    row_at = lax.axis_index("th")
    col_at = lax.axis_index("tw")
    key_local, key_col, key_block = (key_ref[i : i + 1] for i in range(3))
    query_row, query_col, query_peer = (query_ref[:, i : i + 1] for i in range(3))
    key_peer = key_block % 2
    row_limit = jnp.zeros_like(key_local)
    col_limit = jnp.zeros_like(key_local)
    shift = jnp.zeros_like(key_local)
    query_limits = []
    toward = 1 - 2 * (row_at % 2)
    for at, step in enumerate((0, toward, -toward)):
        tile_row = row_at + step
        inside = (tile_row >= 0) & (tile_row < tiles_down)
        tile_row = jnp.clip(tile_row, 0, tiles_down - 1)
        for peer in (0, 1):
            side = 1 - col_at if peer else col_at
            rows = jnp.where(inside, valid_ref[side, 0, tile_row], 0)
            cols = valid_ref[side, 1, tile_row]
            block = 2 * at + peer
            row_limit = jnp.where(key_block == block, rows, row_limit)
            col_limit = jnp.where(key_block == block, cols, col_limit)
            if at == 0:
                query_limits.append((rows, cols))
            else:
                shift = jnp.where(key_block == block, step, shift)
    key_local = key_local + jnp.where(shift < 0, tile_rows - edge_rows, 0)
    key_row = key_local + shift * tile_rows
    key_ok = (key_local < row_limit) & (key_col < col_limit)
    key_at = key_col + tile_cols * jnp.where(key_peer > 0, 1 - col_at, col_at)
    query_at = query_col + tile_cols * jnp.where(query_peer > 0, 1 - col_at, col_at)
    row_gap = jnp.abs(query_row - key_row)
    text = key_block == TEXT_BLOCK
    col_gap = jnp.where(key_ok, jnp.abs(query_at - key_at), 2 * HALO + 1)
    for rows in range(HALO):
        for cols in range(HALO):
            near = (row_gap <= rows + 1) & (col_gap <= cols + 1)
            bias_ref[rows * HALO + cols] = jnp.where(near | text, 0.0, NEG)
    row_limit = jnp.where(query_peer > 0, query_limits[1][0], query_limits[0][0])
    col_limit = jnp.where(query_peer > 0, query_limits[1][1], query_limits[0][1])
    query_ok = (query_row < row_limit) & (query_col < col_limit)
    ok_ref[...] = jnp.broadcast_to(jnp.where(query_ok, 1.0, 0.0), ok_ref.shape)
    step = time_ref[...].astype(jnp.float32)
    step = (step / (1.0 + jnp.exp(-step))).astype(jnp.bfloat16)
    gate = jnp.dot(step, weight_ref[...], preferred_element_type=jnp.float32)
    gate = gate.astype(jnp.bfloat16).astype(jnp.float32)
    for pair in range(gate_ref.shape[0]):
        gate_ref[pair] = gate[0:1, pair * LANES : (pair + 1) * LANES]


def attend_kernel(
    extent_ref,
    mine_q_ref,
    mine_kv_ref,
    peer_ref,
    near_mine_ref,
    far_mine_ref,
    text_ref,
    bias_ref,
    gate_ref,
    ok_ref,
    *refs,
    first_pair,
    pairs,
    unroll,
    score_scale,
):
    near_peer_ref, far_peer_ref, own_out_ref, peer_out_ref, key_ref, value_ref = refs
    count = mine_q_ref.shape[1]
    edge = near_mine_ref.shape[1]
    near = 2 * count + 4 * edge
    first_head = lax.axis_index("tw") * (2 * gate_ref.shape[0])
    left = lax.broadcasted_iota(jnp.int32, (1, LANES), 1) < HEAD_DIM
    zero = jnp.zeros((), jnp.bfloat16)

    def lanes_of(turn):
        start = turn * LANES
        if not isinstance(start, int):
            start = pl.multiple_of(start, LANES)
        return pl.ds(start, LANES)

    def score(turn, slot):
        here, whole = lanes_of(turn), lanes_of(first_pair + turn)
        for part, into in ((0, key_ref.at[slot]), (1, value_ref.at[slot])):
            into[0:count] = mine_kv_ref[part, :, whole]
            into[count : 2 * count] = peer_ref[1 + part, :, here]
            at = 2 * count
            for ref, lanes in (
                (near_mine_ref, whole),
                (near_peer_ref, here),
                (far_mine_ref, whole),
                (far_peer_ref, here),
            ):
                into[at : at + edge] = ref[part, :, lanes]
                at += edge
            into[near:] = text_ref[part, :, whole]
        queries = jnp.concatenate([mine_q_ref[0, :, whole], peer_ref[0, :, here]], 0)
        queries = queries * jnp.asarray(score_scale, jnp.bfloat16)
        queries = jnp.concatenate([jnp.where(left, queries, zero), jnp.where(left, zero, queries)], 0)
        return lax.dot_general(
            queries, key_ref[slot], (((1,), (1,)), ((), ())), preferred_element_type=jnp.float32
        )

    def mix(turn, slot, both):
        here = lanes_of(turn)
        weights, shares = [], []
        for side in (0, 1):
            head = first_head + 2 * (first_pair + turn) + side
            reach_rows = jnp.clip(extent_ref[0, head], 1, HALO) - 1
            reach_cols = jnp.clip(extent_ref[1, head], 1, HALO) - 1
            bias = bias_ref[reach_rows * HALO + reach_cols]
            scores = both[2 * count * side : 2 * count * (side + 1)] + bias
            terms = jnp.exp(scores - jnp.max(scores, axis=-1, keepdims=True))
            shares.append(1.0 / jnp.sum(terms, axis=-1, keepdims=True))
            weights.append(terms.astype(jnp.bfloat16))
        sums = lax.dot_general(
            jnp.concatenate(weights, 0),
            value_ref[slot],
            (((1,), (0,)), ((), ())),
            preferred_element_type=jnp.float32,
        )
        attended = jnp.where(left, sums[: 2 * count] * shares[0], sums[2 * count :] * shares[1])
        gated = jnp.where(ok_ref[...] > 0.0, attended * gate_ref[first_pair + turn], 0.0)
        gated = gated.astype(jnp.bfloat16)
        own_out_ref[:, here] = gated[:count]
        peer_out_ref[:, here] = gated[count:]

    def some_pairs(first, size):
        turns = [(first + slot, slot) for slot in range(size)]
        scored = [score(*turn) for turn in turns]
        for turn, both in zip(turns, scored):
            mix(*turn, both)

    steps = -(-pairs // unroll)
    low, extra = divmod(pairs, steps)
    if extra:
        at = 0
        for step in range(steps):
            some_pairs(at, low + (step < extra))
            at += low + (step < extra)
    else:
        lax.fori_loop(0, steps, lambda step, _: some_pairs(step * low, low), None)


def place_kernel(*refs, moves):
    ins, out_ref, sems = refs[:-2], refs[-2], refs[-1]
    col_at = lax.axis_index("tw")
    half = out_ref.shape[1] // 2
    copies = []
    for at, (source, first, other) in enumerate(moves):
        side = 1 - col_at if other else col_at
        ref = ins[source]
        lanes = pl.ds(pl.multiple_of(side * half + first, LANES), ref.shape[1])
        copies.append(pltpu.make_async_copy(ref, out_ref.at[:, lanes], sems.at[at]))
    for copy in copies:
        copy.start()
    for copy in copies:
        copy.wait()


def place(pieces, base, shape, moves):
    vmem = pl.BlockSpec(memory_space=pltpu.VMEM)
    hbm = pl.BlockSpec(memory_space=pltpu.HBM)
    rest = () if base is None else (base,)
    return pl.pallas_call(
        partial(place_kernel, moves=moves),
        out_shape=jax.ShapeDtypeStruct(shape, jnp.bfloat16),
        in_specs=[vmem] * len(pieces) + [hbm] * len(rest),
        out_specs=hbm,
        scratch_shapes=[pltpu.SemaphoreType.DMA((len(moves),))],
        input_output_aliases={} if base is None else {len(pieces): 0},
        compiler_params=pltpu.CompilerParams(vmem_limit_bytes=VMEM_LIMIT),
    )(*pieces, *rest)


def places(frames, tile_rows, tile_cols, edge, text_count, total):
    groups = frames * tile_cols
    blocks = []
    for at, rows in enumerate((tile_rows, HALO, HALO)):
        shape = (frames, tile_cols, rows)
        row = np.broadcast_to(np.arange(rows), shape).reshape(-1)
        col = np.broadcast_to(np.arange(tile_cols)[:, None], shape).reshape(-1)
        for peer in (0, 1):
            blocks.append(np.stack([row, col, 0 * row + 2 * at + peer]))
            if at:
                blocks.append(np.full((3, edge - groups * HALO), TEXT_BLOCK + 1))
    blocks.append(np.full((3, text_count), TEXT_BLOCK))
    query = np.concatenate([blocks[0], blocks[1]], 1)
    used = sum(block.shape[1] for block in blocks)
    blocks.append(np.full((3, total - used), TEXT_BLOCK + 1))
    keys = np.concatenate([np.concatenate(blocks, 1), np.zeros((5, total))]).astype(np.int32)
    query = np.concatenate([query, np.zeros((5, query.shape[1]))]).T.astype(np.int32)
    top = (np.arange(groups)[:, None] * tile_rows + np.arange(HALO)).reshape(-1)
    bottom = top + tile_rows - HALO
    rest = np.full(edge - groups * HALO, -1)
    chosen = np.stack(
        [np.concatenate([bottom, rest, top, rest]), np.concatenate([top, rest, bottom, rest])]
    )
    select = chosen[:, :, None] == np.arange(groups * tile_rows)
    return keys, query, select.astype(jnp.bfloat16)


def swapped_body(queries, video_kv, text_kv, time_embed, gate_weight, window_extent, tile_valid):
    frames, tile_rows, tile_cols, model_width = queries.shape
    half = model_width // 2
    count = frames * tile_rows * tile_cols
    edge = -(-frames * tile_cols * HALO // 8) * 8
    near_keys = 2 * count + 4 * edge
    text_count = text_kv.shape[1]
    total = -(-(near_keys + text_count) // LANES) * LANES
    text_rows = total - near_keys
    tiles_down = lax.axis_size("th")
    swap = [(0, 1), (1, 0)]
    near_pairs = [(i, i ^ 1) for i in range(tiles_down) if i ^ 1 < tiles_down]
    far_pairs = [(i, ((i + 1) ^ 1) - 1) for i in range(1, tiles_down)]
    far_pairs = [(i, j) for i, j in far_pairs if j < tiles_down]
    cross_pairs = [(2 * i + t, 2 * j + 1 - t) for i, j in far_pairs for t in (0, 1)]
    vmem = pl.BlockSpec(memory_space=pltpu.VMEM)
    smem = pl.BlockSpec(memory_space=pltpu.SMEM)
    params = pltpu.CompilerParams(vmem_limit_bytes=VMEM_LIMIT)
    key_places, query_places, select = places(
        frames, tile_rows, tile_cols, edge, text_count, total
    )
    q = jnp.transpose(queries, (0, 2, 1, 3)).reshape(1, count, model_width)
    kv = jnp.transpose(video_kv, (0, 1, 3, 2, 4)).reshape(2, count, model_width)
    q = pltpu.with_memory_space_constraint(q, pltpu.HBM)
    kv = pltpu.with_memory_space_constraint(kv, pltpu.HBM)
    total_pairs = half // LANES
    pieces = []
    first = 0
    for share in CHUNKS:
        pairs = share * total_pairs // sum(CHUNKS)
        pieces.append((first, pairs))
        first += pairs
    head, tail = slice(0, 1), slice(1, 3)
    (first, pairs), (last, rest) = pieces
    low, width, end = first * LANES, pairs * LANES, rest * LANES
    moves = ((0, low, 0, head, True), (1, low, 0, tail, True))
    (early,) = pack(q, kv, [(3, count, width)], moves)
    arrived = [lax.ppermute(early, "tw", swap)]
    shapes = [(3, count, end), (1, count, half), (2, count, half)]
    low = last * LANES
    moves = (
        (0, 0, 1, slice(0, 1), False),
        (1, 0, 2, slice(0, 2), False),
        (0, low, 0, head, True),
        (1, low, 0, tail, True),
    )
    sent, mine_q, mine_kv = pack(q, kv, shapes, moves)
    near, far, *crossing = pl.pallas_call(
        own_edges_kernel,
        out_shape=[
            jax.ShapeDtypeStruct((2, edge, half), jnp.bfloat16),
            jax.ShapeDtypeStruct((2, edge, half), jnp.bfloat16),
            jax.ShapeDtypeStruct((2, edge, width), jnp.bfloat16),
            jax.ShapeDtypeStruct((2, edge, end), jnp.bfloat16),
        ],
        in_specs=[vmem] * 4,
        out_specs=[vmem] * 4,
        compiler_params=params,
        name="own_edges",
    )(select, mine_kv, early, sent)
    crossed = []
    for rows in crossing:
        crossed.append(lax.ppermute(rows, ("th", "tw"), cross_pairs))
    near_mine = lax.ppermute(near, "th", near_pairs)
    far_mine = lax.ppermute(far, "th", far_pairs)
    arrived.append(lax.ppermute(sent, "tw", swap))
    bias, gate, query_ok = pl.pallas_call(
        partial(
            prepare_kernel,
            tile_rows=tile_rows,
            tile_cols=tile_cols,
            edge_rows=HALO,
            tiles_down=tiles_down,
        ),
        out_shape=[
            jax.ShapeDtypeStruct((HALO * HALO, 2 * count, total), jnp.float32),
            jax.ShapeDtypeStruct((total_pairs, 1, LANES), jnp.float32),
            jax.ShapeDtypeStruct((2 * count, LANES), jnp.float32),
        ],
        in_specs=[smem] + [vmem] * 4,
        out_specs=[vmem] * 3,
        compiler_params=params,
        name="prepare",
    )(
        jnp.transpose(tile_valid.reshape(tiles_down, 2, 2), (1, 2, 0)),
        key_places,
        query_places,
        time_embed.reshape(1, -1),
        gate_weight,
    )
    text = jnp.pad(text_kv, ((0, 0), (0, text_rows - text_count), (0, 0)))
    extents = window_extent.T
    owned, returned = [], []
    for at, ((first, pairs), peer) in enumerate(zip(pieces, arrived)):
        width = pairs * LANES
        far_peer = crossed[at]
        near = pl.pallas_call(
            edges_kernel,
            out_shape=jax.ShapeDtypeStruct((2, edge, width), jnp.bfloat16),
            in_specs=[vmem] * 2 + [pl.BlockSpec(memory_space=pl.ANY)],
            out_specs=vmem,
            compiler_params=params,
        )(select, peer, text)
        near_peer = lax.ppermute(near, "th", near_pairs)
        unroll = min(pairs, UNROLL)
        own_out, peer_out = pl.pallas_call(
            partial(
                attend_kernel,
                first_pair=first,
                pairs=pairs,
                unroll=unroll,
                score_scale=HEAD_DIM ** (-0.5),
            ),
            out_shape=[jax.ShapeDtypeStruct((count, width), jnp.bfloat16)] * 2,
            in_specs=[smem] + [vmem] * 11,
            out_specs=[vmem] * 2,
            scratch_shapes=[pltpu.VMEM((unroll, total, LANES), jnp.bfloat16)] * 2,
            compiler_params=params,
        )(
            extents,
            mine_q,
            mine_kv,
            peer,
            near_mine,
            far_mine,
            text,
            bias,
            gate,
            query_ok,
            near_peer,
            far_peer,
        )
        owned.append(own_out)
        returned.append(lax.ppermute(peer_out, "tw", swap))
    starts = [first * LANES for first, _ in pieces]
    early = owned + returned[:-1]
    moves = [(i, low, False) for i, low in enumerate(starts)]
    moves += [(len(owned) + i, low, True) for i, low in enumerate(starts[:-1])]
    result = place(early, None, (count, model_width), tuple(moves))
    moves = ((0, starts[-1], True),)
    result = place(returned[-1:], result, (count, model_width), moves)
    result = result.reshape(frames, tile_cols, tile_rows, model_width)
    return jnp.transpose(result, (0, 2, 1, 3))


def solution(mesh):
    placed = (
        P("vid", "th", "tw", None),
        P(None, "vid", "th", "tw", None),
        P(None, "vid", "tw"),
        P("vid"),
        P(None, "tw"),
        P(),
        P("vid", None, None),
    )
    swapped = mesh.shape["tw"] == 2
    body = swapped_body if swapped else general_body

    return jax.shard_map(
        body, mesh=mesh, in_specs=placed, out_specs=P("vid", "th", "tw", None), check_vma=False
    )
```
